128 devices in a mesh: pair: 64 (over x, y, z), rep: 2 (over core).
Axes of the slice: x: 4, y: 4, z: 4, core: 2. Of those that a mesh axis runs over, the one named last changes fastest.
Arguments:
- triplet_pairs: int32 [1024, 3], P(('pair', 'rep')), may hold values from 0 to 4095, as said below
- tno_width: int32 [1024], P(('pair', 'rep')), may hold values from 64 to 128
- pair_width: int32 [4096], P('pair'), may hold values from 32 to 64
- pair_coeff: bfloat16 [4096, 64, 1024], P('pair'), may hold values from -0.1875 to 0.1875
- pair_amps: bfloat16 [4096, 64, 64], P('pair'), may hold values from -0.03125 to 0.03125
- pair_exch: bfloat16 [4096, 64, 64], P('pair'), may hold values from -0.3125 to 0.3125
- tno_coeff: bfloat16 [1024, 1024, 128], P(('pair', 'rep')), may hold values from -0.1875 to 0.1875
- int_left: bfloat16 [1024, 3, 128, 128], P(('pair', 'rep')), may hold values from -6 to 6
- int_right: bfloat16 [1024, 3, 128, 128], P(('pair', 'rep')), may hold values from -6 to 6
- singles: float32 [1024, 3, 128], P(('pair', 'rep')), may hold values from -6 to 6
- tno_energy: float32 [1024, 128], P(('pair', 'rep')), may hold values from 0.5 to 5
- gap: float32 [1024], P(('pair', 'rep')), may hold values from 1 to 4
Outputs:
- triplet_energy: float32 [1024], P(('pair', 'rep'))
- pair_energy: float32 [4096], P('pair')
The draws below stay inside these ranges and needn't reach their ends.
Inputs may be any that keep to these rules, and one draw needn't show every extreme that they name: `triplet_pairs`: pair p is owned by index p // 64 of axis pair. The triplets of one chip are rows 2 * c * 8 to 2 * (c + 1) * 8 - 1; among their 48 pair ids at most 1 have one owner, and in every chip some owner has exactly 1 of them.
All inputs are finite; a program needn't handle non-finite values.
Results may differ from the reference program's by a relative error of at most 0.00044.
Values may be sent and summed in bfloat16 or wider, within the bound.
No kernel may reach another device: no remote copies, remote signals or barrier semaphores. Data moves between devices by JAX's collectives and lax.ppermute only.
A program may use at most 128 MiB of HBM per device.

```python
import math
import jax
import jax.numpy as jnp
from jax import lax

TRIP_DEV = 8
PAIR_DEV = 64
A = 64
B = 128
DOM = 1024
TRIPLETS = 1024
PAIRS = 4096
N_PAIR = 64


def draw_triplet_pairs(key, part):
    references = 6 * TRIP_DEV
    per_owner = (references + N_PAIR - 1) // N_PAIR
    half_len = references // 2

    def one_chip(chip_key):
        key_list = jax.random.split(chip_key, per_owner + 4)
        permuted = jnp.concatenate([jax.random.permutation(key_list[turn], N_PAIR).astype(jnp.int32) for turn in range(per_owner)])
        owners = permuted[:references]
        hottest = permuted[(per_owner - 1) * N_PAIR]
        position = jnp.arange(references, dtype=jnp.int32)
        reorder = jnp.argsort(jnp.where(owners == hottest, 0, references) + position)
        owners = owners[reorder]
        first_half = owners[:half_len][jax.random.permutation(key_list[per_owner], half_len)]
        second_half = owners[half_len:][jax.random.permutation(key_list[per_owner + 1], half_len)]
        flipped = jax.random.randint(key_list[per_owner + 2], (), 0, 2)
        owners = jnp.where(flipped == 1, jnp.concatenate([second_half, first_half]), jnp.concatenate([first_half, second_half]))
        local_rows = jax.random.randint(key_list[per_owner + 3], (references,), 0, PAIR_DEV)
        return (owners * PAIR_DEV + local_rows).astype(jnp.int32)
    pair_ids = jax.vmap(one_chip)(jax.random.split(jax.random.fold_in(key, 7), N_PAIR))
    return pair_ids.reshape(TRIPLETS, 3)


def plant(values, key, smallest, high):
    longest = values.shape.index(max(values.shape))
    spots = []
    for shift in (0, 1):
        where = [jax.random.randint(jax.random.fold_in(key, axis), (), 0, length) for axis, length in enumerate(values.shape)]
        where[longest] = (where[longest] + shift) % values.shape[longest]
        spots.append(tuple(where))
    return values.at[spots[0]].set(smallest).at[spots[1]].set(high)


def level_of(key, shape, cuts, smallest, top_value):
    gain, own = 1.0, jax.random.fold_in(key, 6)
    for dim, parts in cuts:
        draws = jnp.exp(jax.random.uniform(jax.random.fold_in(own, dim), (parts,), jnp.float32, smallest / len(cuts), top_value / len(cuts)))
        gain = gain * jnp.repeat(draws, shape[dim] // parts).reshape([-1 if axis == dim else 1 for axis in range(len(shape))])
    return gain


def centred(own_key, extent, width, bound, cuts=(), kind=jnp.bfloat16):
    entries = width * jax.random.normal(own_key, extent, jnp.float32)
    if cuts:
        entries = entries * level_of(own_key, extent, cuts, -0.22, 0.18)
    return jnp.clip(entries, -bound, bound).astype(kind)


def setup_inputs(seed: int = 0) -> dict:
    keys = jax.random.split(jax.random.key(seed), 13)
    triplet_pairs = draw_triplet_pairs(jax.random.fold_in(keys[12], 71), 0)
    tno_width = plant(jax.random.randint(keys[1], (TRIPLETS,), B // 2, B + 1), jax.random.fold_in(keys[1], 1), B // 2, B).astype(jnp.int32)
    pair_width = plant(jax.random.randint(keys[2], (PAIRS,), A // 2, A + 1), jax.random.fold_in(keys[2], 1), A // 2, A).astype(jnp.int32)
    pair_coeff = centred(keys[3], (PAIRS, A, DOM), DOM ** -0.5, 0.1875, ((0, 64),))
    pair_amps = centred(keys[4], (PAIRS, A, A), (2.0 * DOM / (A * B * B)), 0.03125, ((0, 64),))
    pair_exch = centred(keys[5], (PAIRS, A, A), (20.0 * DOM / (A * B * B)), 0.3125, ((0, 64),))
    tno_coeff = centred(keys[6], (TRIPLETS, DOM, B), DOM ** -0.5, 0.1875, ((0, 128),))
    int_left = centred(keys[7], (TRIPLETS, 3, B, B), 1.0, 6.0, ((0, 128),))
    int_right = centred(keys[8], (TRIPLETS, 3, B, B), 1.0, 6.0, ((0, 128),))
    singles = centred(keys[9], (TRIPLETS, 3, B), 0.5, 6.0, ((0, 128),), jnp.float32)
    tno_energy = jnp.clip(jnp.exp(math.log(5.0) - 2.3025851 * jax.random.uniform(keys[10], (TRIPLETS, B), jnp.float32) ** level_of(keys[10], (TRIPLETS, B), ((0, 128),), -0.2, 0.2)), 0.5, 5.0)
    gap = jnp.clip(jnp.exp(math.log(4.0) - 1.3862944 * jax.random.uniform(keys[11], (TRIPLETS,), jnp.float32) ** level_of(keys[11], (TRIPLETS,), ((0, 128),), -0.2, 0.2)), 1.0, 4.0)
    return dict(triplet_pairs=triplet_pairs, tno_width=tno_width, pair_width=pair_width, pair_coeff=pair_coeff, pair_amps=pair_amps, pair_exch=pair_exch, tno_coeff=tno_coeff, int_left=int_left, int_right=int_right, singles=singles, tno_energy=tno_energy, gap=gap)


def projected_energy(pno_coeff, pno_blocks, tno_block, tno_count, left, right, single_amps, tno_levels, shift):
    tno_size = tno_block.shape[1]
    pno_size = pno_coeff.shape[1]
    kept_cols = (jnp.arange(tno_size, dtype=jnp.int32) < tno_count).astype(jnp.float32)
    tno_kept = tno_block.astype(jnp.float32) * kept_cols[None, :]
    intersection = lax.optimization_barrier(jnp.einsum('xad,db->xab', pno_coeff.astype(jnp.float32), tno_kept).astype(jnp.bfloat16))
    halfway = jnp.einsum('xab,xac->xbc', intersection.astype(jnp.float32), pno_blocks.astype(jnp.float32))
    halfway = lax.optimization_barrier(halfway.astype(jnp.bfloat16)).reshape(3, tno_size, 2, pno_size)
    projected = jnp.einsum('xbkc,xcd->xkbd', halfway.astype(jnp.float32), intersection.astype(jnp.float32))
    amps_tno = lax.optimization_barrier(projected[:, 0].astype(jnp.bfloat16))
    exch_tno = projected[:, 1]
    khatri = left.astype(jnp.float32)[:, :, :, None] * right.astype(jnp.float32)[:, :, None, :]
    khatri = lax.optimization_barrier(khatri.astype(jnp.bfloat16))
    expanded = khatri.reshape(3 * tno_size, tno_size * tno_size)
    leading = jnp.transpose(amps_tno, (1, 0, 2)).reshape(tno_size, 3 * tno_size)
    connected = jnp.dot(leading, expanded, preferred_element_type=jnp.float32).reshape(tno_size, tno_size, tno_size)
    complete = connected + single_amps[0][None, None, :] * exch_tno[0][:, :, None]
    complete = complete + single_amps[1][None, :, None] * exch_tno[1][:, None, :]
    complete = complete + single_amps[2][:, None, None] * exch_tno[2][None, :, :]
    denominator = tno_levels[:, None, None] + tno_levels[None, :, None] + tno_levels[None, None, :] + shift
    cube_mask = kept_cols[:, None, None] * kept_cols[None, :, None] * kept_cols[None, None, :]
    return jnp.sum(cube_mask * connected * complete / denominator)


def reference(triplet_pairs, tno_width, pair_width, pair_coeff, pair_amps, pair_exch, tno_coeff, int_left, int_right, singles, tno_energy, gap):
    kept_rows = (jnp.arange(A, dtype=jnp.int32)[None, :] < pair_width[:, None]).astype(jnp.float32)
    masked = (pair_coeff.astype(jnp.float32) * kept_rows[:, :, None]).astype(jnp.bfloat16)
    paired = jnp.concatenate([pair_amps, pair_exch], axis=2)

    def single_triplet(index):
        pair_ids = triplet_pairs[index]
        return projected_energy(masked[pair_ids], paired[pair_ids], tno_coeff[index], tno_width[index], int_left[index], int_right[index], singles[index], tno_energy[index], gap[index])

    energies = lax.map(single_triplet, jnp.arange(TRIPLETS, dtype=jnp.int32))
    shares = jnp.repeat(energies / 3.0, 3)
    pair_energy = jax.ops.segment_sum(shares, triplet_pairs.reshape(-1), num_segments=PAIRS)
    return energies, pair_energy
```

```python
import jax
import jax.numpy as jnp
from jax import lax
from jax.experimental import pallas as pl
from jax.experimental.pallas import tpu as pltpu
from jax.sharding import PartitionSpec as P

BOTH = ("pair", "rep")


def slots_kernel(rows, coeff, blocks, out, buf, got, put, *, halves):
    slots, slot_rows, lanes = buf.shape
    pno = coeff.shape[1]
    dom_part = coeff.shape[2] // halves
    pieces = dom_part // lanes
    pair_rows = pno // halves
    rep = rows[slots]

    def start(s, _):
        row = rows[s]
        for piece in range(pieces):
            pltpu.make_async_copy(
                coeff.at[row, :, pl.ds(rep * dom_part + piece * lanes, lanes)],
                buf.at[s, pl.ds(piece * pno, pno), :],
                got.at[s],
            ).start()
        pltpu.make_async_copy(
            blocks.at[row, pl.ds(rep * pair_rows, pair_rows), :],
            buf.at[s, pl.ds(pieces * pno, pair_rows), :],
            got.at[s],
        ).start()
        return 0

    def forward(s, _):
        pltpu.make_async_copy(out.at[s], buf.at[s], got.at[s]).wait()
        pltpu.make_async_copy(buf.at[s], out.at[s], put.at[s]).start()
        return 0

    def finish(s, _):
        pltpu.make_async_copy(buf.at[s], out.at[s], put.at[s]).wait()
        return 0

    lax.fori_loop(0, slots, start, 0)
    lax.fori_loop(0, slots, forward, 0)
    lax.fori_loop(0, slots, finish, 0)


def send_slots(rows, coeff, blocks, halves):
    slots = rows.shape[0] - 1
    _, pno, domain = coeff.shape
    lanes = blocks.shape[2]
    slot_rows = pno * (domain // halves // lanes) + pno // halves
    shape = (slots, slot_rows, lanes)
    return pl.pallas_call(
        lambda *refs: slots_kernel(*refs, halves=halves),
        grid_spec=pltpu.PrefetchScalarGridSpec(
            num_scalar_prefetch=1,
            grid=(),
            in_specs=[pl.BlockSpec(memory_space=pl.ANY), pl.BlockSpec(memory_space=pl.ANY)],
            out_specs=pl.BlockSpec(memory_space=pl.ANY),
            scratch_shapes=[
                pltpu.VMEM(shape, jnp.bfloat16),
                pltpu.SemaphoreType.DMA((slots,)),
                pltpu.SemaphoreType.DMA((slots,)),
            ],
        ),
        out_shape=jax.ShapeDtypeStruct(shape, jnp.bfloat16),
        name="slots",
    )(rows, coeff, blocks)


def dot_nt(x, y):
    return lax.dot_general(x, y, (((1,), (1,)), ((), ())), preferred_element_type=jnp.float32)


def dot_tn(x, y):
    return lax.dot_general(x, y, (((0,), (0,)), ((), ())), preferred_element_type=jnp.float32)


def dot_tt(x, y):
    return lax.dot_general(x, y, (((0,), (1,)), ((), ())), preferred_element_type=jnp.float32)


def down_rows(row):
    size = row.shape[1]
    return jnp.transpose(jnp.broadcast_to(row, (size, size)))


STEP = 8


def energy_kernel(
    meta, levels_s, singles_s, gap_s,
    own0, own1, own2, far0, far1, far2, tno, left, right, singles, levels,
    out,
    left_t, right_t, weights, exch0, exch1, exch2, single0, base, ix,
):
    t = pl.program_id(0)
    trips = levels_s.shape[0]
    width = meta[4 * trips - trips + t]
    rep = meta[4 * trips]
    own = (own0, own1, own2)
    far = (far0, far1, far2)
    size = tno.shape[2]
    half_dom = tno.shape[1] // 2
    lanes = own0.shape[2]
    pieces = half_dom // lanes
    pno = (own0.shape[1] * 2) // (2 * pieces + 1)
    part = pno // 2

    def stacked(refs):
        rows = []
        for ref in refs:
            cols = [ref[0, k * pno : (k + 1) * pno, :] for k in range(pieces)]
            rows.append(jnp.concatenate(cols, axis=1))
        return jnp.concatenate(rows, axis=0)

    inter = jnp.dot(
        stacked(own), tno[0, pl.ds(rep * half_dom, half_dom), :], preferred_element_type=jnp.float32
    )
    inter += jnp.dot(
        stacked(far),
        tno[0, pl.ds((1 - rep) * half_dom, half_dom), :],
        preferred_element_type=jnp.float32,
    )
    lane = lax.broadcasted_iota(jnp.int32, inter.shape, 1)
    inter = jnp.where(lane < width, inter, 0.0).astype(jnp.bfloat16)
    row_ok = lax.broadcasted_iota(jnp.int32, (size, size), 0) < width
    eye = (
        lax.broadcasted_iota(jnp.int32, (size, size), 0)
        == lax.broadcasted_iota(jnp.int32, (size, size), 1)
    ).astype(jnp.float32).astype(jnp.bfloat16)
    weights[...] = jnp.zeros(weights.shape, weights.dtype)
    exch = (exch0, exch1, exch2)
    spots = ((0, 256), (128, 384), (512, 640))
    for x in range(3):
        ix[pl.ds(rep * part, part), :] = own[x][0, pieces * pno : pieces * pno + part, :]
        ix[pl.ds((1 - rep) * part, part), :] = far[x][0, pieces * pno : pieces * pno + part, :]
        inter_x = inter[x * pno : (x + 1) * pno, :]
        halfway = dot_tn(inter_x, ix[...]).astype(jnp.bfloat16)
        amps = dot_tt(inter_x, halfway[:, :pno]).astype(jnp.bfloat16)
        exch[x][...] = dot_tt(inter_x, halfway[:, pno:])
        weights[spots[x][0] : spots[x][0] + size, :size] = amps
        weights[spots[x][1] : spots[x][1] + size, size:] = amps
        left_t[:, x * size : (x + 1) * size] = jnp.where(row_ok, dot_nt(eye, left[0, x]), 0.0)
        right_t[:, x * size : (x + 1) * size] = jnp.where(
            row_ok, dot_nt(eye, right[0, x]), 0.0
        ).astype(jnp.bfloat16)
    single0[...] = down_rows(singles[0, 0:1, :])
    base[...] = down_rows(levels[0, 0:1, :]) + levels[0, 0:1, :] + gap_s[t]
    single2 = singles[0, 2:3, :]

    def block(i, total):
        b0 = i * STEP
        left_rows = left_t[pl.ds(b0, STEP), :]
        exch0_rows = exch0[pl.ds(b0, STEP), :]
        exch2_cols = pltpu.roll(exch2[...], size - b0, 1)
        right_all = right_t[...]
        for j in range(0, STEP, 2):
            first = right_all * jnp.broadcast_to(left_rows[j : j + 1, :], right_all.shape).astype(
                jnp.bfloat16
            )
            second = right_all * jnp.broadcast_to(
                left_rows[j + 1 : j + 2, :], right_all.shape
            ).astype(jnp.bfloat16)
            khatri = jnp.concatenate(
                [first[:, :256], second[:, :256], first[:, 256:], second[:, 256:]], axis=1
            )
            both = jnp.dot(khatri, weights[...], preferred_element_type=jnp.float32)
            for h in range(2):
                b = b0 + j + h
                connected = both[:, h * size : (h + 1) * size]
                complete = connected + singles_s[t, 1, b] * exch1[...]
                complete += single0[...] * exch0_rows[j + h : j + h + 1, :]
                complete += exch2_cols[:, j + h : j + h + 1] * single2
                term = connected * complete / (base[...] + levels_s[t, b])
                total += jnp.sum(term.reshape(size // 8, 8, size), axis=0)
        return total

    blocks = (width + STEP - 1) // STEP
    out[0] = lax.fori_loop(0, blocks, block, jnp.zeros((8, size), jnp.float32))


def triplet_energies(meta, own, far, tno, left, right, singles, levels, gap):
    trips, _, size = tno.shape
    slot = own.shape[1:]

    def pair_spec(x):
        return pl.BlockSpec((1, *slot), lambda t, meta, *_: (meta[3 * t + x], 0, 0))

    def trip_spec(shape):
        return pl.BlockSpec((1, *shape), lambda t, *_: (t,) + (0,) * len(shape))

    return pl.pallas_call(
        energy_kernel,
        grid_spec=pltpu.PrefetchScalarGridSpec(
            num_scalar_prefetch=4,
            grid=(trips,),
            in_specs=[pair_spec(x) for x in range(3)]
            + [pair_spec(x) for x in range(3)]
            + [
                trip_spec(tno.shape[1:]),
                trip_spec(left.shape[1:]),
                trip_spec(right.shape[1:]),
                trip_spec(singles.shape[1:]),
                trip_spec((1, size)),
            ],
            out_specs=trip_spec((8, size)),
            scratch_shapes=[
                pltpu.VMEM((size, 3 * size), jnp.float32),
                pltpu.VMEM((size, 3 * size), jnp.bfloat16),
                pltpu.VMEM((6 * size, 2 * size), jnp.bfloat16),
                pltpu.VMEM((size, size), jnp.float32),
                pltpu.VMEM((size, size), jnp.float32),
                pltpu.VMEM((size, size), jnp.float32),
                pltpu.VMEM((size, size), jnp.float32),
                pltpu.VMEM((size, size), jnp.float32),
                pltpu.VMEM((size // 2, size), jnp.bfloat16),
            ],
        ),
        out_shape=jax.ShapeDtypeStruct((trips, 8, size), jnp.float32),
        compiler_params=pltpu.CompilerParams(dimension_semantics=("arbitrary",)),
        name="energy",
    )(
        meta, levels, singles, gap,
        own, own, own, far, far, far, tno, left, right, singles, levels.reshape(trips, 1, size),
    )


def body(
    triplet_pairs, tno_width, pair_width, pair_coeff, pair_amps, pair_exch, tno_coeff,
    int_left, int_right, singles, tno_energy, gap,
):
    owners_n = lax.axis_size("pair")
    reps = lax.axis_size("rep")
    pair_dev, pno, _ = pair_coeff.shape
    rep = lax.axis_index("rep")
    references = triplet_pairs.reshape(-1)
    owners = references // pair_dev
    at_owner = owners[None, :] == jnp.arange(owners_n, dtype=jnp.int32)[:, None]

    wanted = jnp.sum(jnp.where(at_owner, references % pair_dev + 1, 0), axis=1)
    wanted = jnp.broadcast_to(wanted[:, None], (owners_n, reps)).reshape(-1, 1)
    asked = lax.all_to_all(wanted, BOTH, 0, 0, tiled=True)
    asked = jnp.max(asked.reshape(owners_n, reps), axis=1) - 1

    kept = jnp.arange(pno, dtype=jnp.int32)[None, :] < pair_width[:, None]
    kept = kept[:, :, None] & kept[:, None, :]
    zero = jnp.zeros((), pair_amps.dtype)
    blocks = jnp.concatenate(
        [jnp.where(kept, pair_amps, zero), jnp.where(kept, pair_exch, zero)], axis=2
    )
    rows = jnp.concatenate([jnp.maximum(asked, 0), rep[None].astype(jnp.int32)])
    sent = send_slots(rows, pair_coeff, blocks, reps)
    got = lax.all_to_all(sent, "pair", 0, 0, tiled=True)
    far = lax.ppermute(got, "rep", [(0, 1), (1, 0)])

    meta = jnp.concatenate([owners, tno_width, rep[None].astype(jnp.int32)])
    partial = triplet_energies(
        meta, got, far, tno_coeff, int_left, int_right, singles, tno_energy, gap
    )
    energies = jnp.sum(partial, axis=(1, 2))

    shares = jnp.repeat(energies / 3.0, 3)
    shares = jnp.sum(jnp.where(at_owner, shares[None, :], 0.0), axis=1)
    shares = jnp.broadcast_to(shares[:, None], (owners_n, reps)).reshape(-1, 1)
    shares = lax.all_to_all(shares, BOTH, 0, 0, tiled=True)
    shares = jnp.sum(shares.reshape(owners_n, reps), axis=1)
    here = asked[None, :] == jnp.arange(pair_dev, dtype=jnp.int32)[:, None]
    pair_energy = jnp.sum(jnp.where(here, shares[None, :], 0.0), axis=1)
    return (energies, pair_energy)


def solution(mesh):
    both = P(BOTH)
    pair = P("pair")
    placed = (both, both, pair, pair, pair, pair, both, both, both, both, both, both)
    return jax.shard_map(
        body, mesh=mesh, in_specs=placed, out_specs=(both, pair), check_vma=False
    )
```

```python
import jax
import jax.numpy as jnp
from jax import lax
from jax.experimental import pallas as pl
from jax.experimental.pallas import tpu as pltpu
from jax.sharding import PartitionSpec as P

BOTH = ("pair", "rep")


def slots_kernel(rows, coeff, blocks, out, buf, got, put, *, halves):
    slots, slot_rows, lanes = buf.shape
    pno = coeff.shape[1]
    dom_part = coeff.shape[2] // halves
    pieces = dom_part // lanes
    pair_rows = pno // halves
    rep = rows[slots]

    def start(s, _):
        row = rows[s]
        for piece in range(pieces):
            pltpu.make_async_copy(
                coeff.at[row, :, pl.ds(rep * dom_part + piece * lanes, lanes)],
                buf.at[s, pl.ds(piece * pno, pno), :],
                got.at[s],
            ).start()
        pltpu.make_async_copy(
            blocks.at[row, pl.ds(rep * pair_rows, pair_rows), :],
            buf.at[s, pl.ds(pieces * pno, pair_rows), :],
            got.at[s],
        ).start()
        return 0

    def forward(s, _):
        pltpu.make_async_copy(out.at[s], buf.at[s], got.at[s]).wait()
        pltpu.make_async_copy(buf.at[s], out.at[s], put.at[s]).start()
        return 0

    def finish(s, _):
        pltpu.make_async_copy(buf.at[s], out.at[s], put.at[s]).wait()
        return 0

    lax.fori_loop(0, slots, start, 0)
    lax.fori_loop(0, slots, forward, 0)
    lax.fori_loop(0, slots, finish, 0)


def send_slots(rows, coeff, blocks, halves):
    slots = rows.shape[0] - 1
    _, pno, domain = coeff.shape
    lanes = blocks.shape[2]
    slot_rows = pno * (domain // halves // lanes) + pno // halves
    shape = (slots, slot_rows, lanes)
    return pl.pallas_call(
        lambda *refs: slots_kernel(*refs, halves=halves),
        grid_spec=pltpu.PrefetchScalarGridSpec(
            num_scalar_prefetch=1,
            grid=(),
            in_specs=[pl.BlockSpec(memory_space=pl.ANY), pl.BlockSpec(memory_space=pl.ANY)],
            out_specs=pl.BlockSpec(memory_space=pl.ANY),
            scratch_shapes=[
                pltpu.VMEM(shape, jnp.bfloat16),
                pltpu.SemaphoreType.DMA((slots,)),
                pltpu.SemaphoreType.DMA((slots,)),
            ],
        ),
        out_shape=jax.ShapeDtypeStruct(shape, jnp.bfloat16),
        name="slots",
    )(rows, coeff, blocks)


def dot_nt(x, y):
    return lax.dot_general(x, y, (((1,), (1,)), ((), ())), preferred_element_type=jnp.float32)


def dot_tn(x, y):
    return lax.dot_general(x, y, (((0,), (0,)), ((), ())), preferred_element_type=jnp.float32)


def dot_tt(x, y):
    return lax.dot_general(x, y, (((0,), (1,)), ((), ())), preferred_element_type=jnp.float32)


def down_rows(row):
    size = row.shape[1]
    return jnp.transpose(jnp.broadcast_to(row, (size, size)))


STEP = 8
GROUP = 2


def prepare_kernel(widths, gap_s, left, right, singles, levels, left_t, right_t, columns):
    t = pl.program_id(0)
    size = left.shape[2]
    rows = lax.broadcasted_iota(jnp.int32, (size, size), 0)
    row_ok = rows < widths[t]
    eye = (rows == lax.broadcasted_iota(jnp.int32, (size, size), 1)).astype(jnp.float32)
    eye = eye.astype(jnp.bfloat16)
    for x in range(3):
        left_t[0, x] = jnp.where(row_ok, dot_nt(eye, left[0, x]), 0.0)
        right_t[0, x] = jnp.where(row_ok, dot_nt(eye, right[0, x]), 0.0)
    columns[0, 0] = down_rows(singles[0, 0:1, :])
    columns[0, 1] = down_rows(levels[0, 0:1, :]) + levels[0, 0:1, :] + gap_s[t]


def trip_spec(shape):
    return pl.BlockSpec((1, *shape), lambda t, *_: (t,) + (0,) * len(shape))


def prepare(widths, gap, left, right, singles, levels):
    trips, _, size, _ = left.shape
    return pl.pallas_call(
        prepare_kernel,
        grid_spec=pltpu.PrefetchScalarGridSpec(
            num_scalar_prefetch=2,
            grid=(trips,),
            in_specs=[
                trip_spec(left.shape[1:]),
                trip_spec(right.shape[1:]),
                trip_spec(singles.shape[1:]),
                trip_spec((1, size)),
            ],
            out_specs=[
                trip_spec((3, size, size)),
                trip_spec((3, size, size)),
                trip_spec((2, size, size)),
            ],
        ),
        out_shape=[
            jax.ShapeDtypeStruct((trips, 3, size, size), jnp.float32),
            jax.ShapeDtypeStruct((trips, 3, size, size), jnp.float32),
            jax.ShapeDtypeStruct((trips, 2, size, size), jnp.float32),
        ],
        compiler_params=pltpu.CompilerParams(dimension_semantics=("arbitrary",)),
        cost_estimate=pl.CostEstimate(
            flops=12 * trips * size**3, bytes_accessed=8 * trips * size**2 * 4, transcendentals=0
        ),
        name="prepare",
    )(widths, gap, left, right, singles, levels.reshape(trips, 1, size))


def energy_kernel(
    meta, levels_s, singles_s,
    own0, own1, own2, far0, far1, far2, tno, left_t, right_t, columns, singles,
    out,
    weights, exch0, exch1, exch2, connected_s, ix,
):
    t = pl.program_id(0)
    trips = levels_s.shape[0]
    width = meta[3 * trips + t]
    rep = meta[4 * trips]
    own = (own0, own1, own2)
    far = (far0, far1, far2)
    size = tno.shape[2]
    half_dom = tno.shape[1] // 2
    lanes = own0.shape[2]
    pieces = half_dom // lanes
    pno = (own0.shape[1] * 2) // (2 * pieces + 1)
    part = pno // 2
    pairs = STEP // 2

    def stacked(refs):
        rows = []
        for ref in refs:
            cols = [ref[0, k * pno : (k + 1) * pno, :] for k in range(pieces)]
            rows.append(jnp.concatenate(cols, axis=1))
        return jnp.concatenate(rows, axis=0)

    inter = jnp.dot(
        stacked(own), tno[0, pl.ds(rep * half_dom, half_dom), :], preferred_element_type=jnp.float32
    )
    inter += jnp.dot(
        stacked(far),
        tno[0, pl.ds((1 - rep) * half_dom, half_dom), :],
        preferred_element_type=jnp.float32,
    )
    lane = lax.broadcasted_iota(jnp.int32, inter.shape, 1)
    inter = jnp.where(lane < width, inter, 0.0).astype(jnp.bfloat16)

    @pl.when(t == 0)
    def _():
        weights[...] = jnp.zeros(weights.shape, weights.dtype)

    exch = (exch0, exch1, exch2)
    spots = ((0, 256), (128, 384), (512, 640))
    for x in range(3):
        ix[x, pl.ds(rep * part, part), :] = own[x][0, pieces * pno : pieces * pno + part, :]
        ix[x, pl.ds((1 - rep) * part, part), :] = far[x][0, pieces * pno : pieces * pno + part, :]
    for x in range(3):
        inter_x = inter[x * pno : (x + 1) * pno, :]
        halfway = dot_tn(inter_x, ix[x]).astype(jnp.bfloat16)
        amps = dot_tt(inter_x, halfway[:, :pno]).astype(jnp.bfloat16)
        exch[x][...] = dot_tt(inter_x, halfway[:, pno:])
        weights[spots[x][0] : spots[x][0] + size, :size] = amps
        weights[spots[x][1] : spots[x][1] + size, size:] = amps
    single2 = singles[0, 2:3, :]

    def with_rows(m):
        def connect(i):
            b0 = i * STEP
            right_x = [right_t[0, x, :m, :].astype(jnp.bfloat16) for x in range(3)]
            left_x = [left_t[0, x, pl.ds(b0, STEP), :] for x in range(3)]

            def product(x, j):
                row = jnp.broadcast_to(left_x[x][j : j + 1, :], (m, size)).astype(jnp.bfloat16)
                return right_x[x] * row

            for group in range(0, pairs, GROUP):
                khatri = jnp.concatenate(
                    [
                        jnp.concatenate(
                            [
                                product(0, j), product(1, j), product(0, j + 1), product(1, j + 1),
                                product(2, j), product(2, j + 1),
                            ],
                            axis=1,
                        )
                        for j in range(2 * group, 2 * (group + GROUP), 2)
                    ],
                    axis=0,
                )
                both = jnp.dot(khatri, weights[...], preferred_element_type=jnp.float32)
                for k in range(GROUP):
                    connected_s[group + k, :m, :] = both[k * m : (k + 1) * m, :]

        def energies(i, total):
            b0 = i * STEP
            exch0_rows = exch0[pl.ds(b0, STEP), :]
            exch2_cols = pltpu.roll(exch2[:m, :], size - b0, 1)
            for j in range(STEP):
                connected = connected_s[j // 2, :m, (j % 2) * size : (j % 2 + 1) * size]
                complete = connected + singles_s[t, 1, b0 + j] * exch1[:m, :]
                complete += columns[0, 0, :m, :] * exch0_rows[j : j + 1, :]
                complete += exch2_cols[:, j : j + 1] * single2
                term = connected * complete / (columns[0, 1, :m, :] + levels_s[t, b0 + j])
                total += jnp.sum(term.reshape(m // 8, 8, size), axis=0)
            return total

        def block(i, total):
            total = energies(i, total)
            connect(i + 1)
            return total

        blocks = (width + STEP - 1) // STEP
        connect(0)
        total = lax.fori_loop(0, blocks - 1, block, jnp.zeros((8, size), jnp.float32))
        out[0] = energies(blocks - 1, total)

    needed = (width + 15) // 16 * 16
    for m in range(size // 2, size + 1, 16):
        pl.when(needed == m)(lambda m=m: with_rows(m))


def triplet_energies(meta, own, far, tno, left_t, right_t, columns, singles, levels):
    trips, _, size = tno.shape
    slot = own.shape[1:]
    pno = slot[0] * 2 // (tno.shape[1] // slot[1] + 1)

    def pair_spec(x):
        return pl.BlockSpec((1, *slot), lambda t, meta, *_: (meta[3 * t + x], 0, 0))

    return pl.pallas_call(
        energy_kernel,
        grid_spec=pltpu.PrefetchScalarGridSpec(
            num_scalar_prefetch=3,
            grid=(trips,),
            in_specs=[pair_spec(x) for x in range(3)]
            + [pair_spec(x) for x in range(3)]
            + [
                trip_spec(tno.shape[1:]),
                trip_spec(left_t.shape[1:]),
                trip_spec(right_t.shape[1:]),
                trip_spec(columns.shape[1:]),
                trip_spec(singles.shape[1:]),
            ],
            out_specs=trip_spec((8, size)),
            scratch_shapes=[
                pltpu.VMEM((6 * size, 2 * size), jnp.bfloat16),
                pltpu.VMEM((size, size), jnp.float32),
                pltpu.VMEM((size, size), jnp.float32),
                pltpu.VMEM((size, size), jnp.float32),
                pltpu.VMEM((STEP // 2, size, 2 * size), jnp.float32),
                pltpu.VMEM((3, pno, 2 * pno), jnp.bfloat16),
            ],
        ),
        out_shape=jax.ShapeDtypeStruct((trips, 8, size), jnp.float32),
        compiler_params=pltpu.CompilerParams(dimension_semantics=("arbitrary",)),
        name="energy",
    )(meta, levels, singles, own, own, own, far, far, far, tno, left_t, right_t, columns, singles)


def test_entry(meta, own, far, tno, left, right, singles, levels, gap):
    trips = tno.shape[0]
    ready = prepare(meta[3 * trips : 4 * trips], gap, left, right, singles, levels)
    return jnp.sum(triplet_energies(meta, own, far, tno, *ready, singles, levels), axis=(1, 2))


def body(
    triplet_pairs, tno_width, pair_width, pair_coeff, pair_amps, pair_exch, tno_coeff,
    int_left, int_right, singles, tno_energy, gap,
):
    owners_n = lax.axis_size("pair")
    reps = lax.axis_size("rep")
    pair_dev, pno, _ = pair_coeff.shape
    rep = lax.axis_index("rep")
    references = triplet_pairs.reshape(-1)
    owners = references // pair_dev
    at_owner = owners[None, :] == jnp.arange(owners_n, dtype=jnp.int32)[:, None]

    wanted = jnp.sum(jnp.where(at_owner, references % pair_dev + 1, 0), axis=1)
    wanted = jnp.broadcast_to(wanted[:, None], (owners_n, reps)).reshape(-1, 1)
    asked = lax.all_to_all(wanted, BOTH, 0, 0, tiled=True)
    asked = jnp.max(asked.reshape(owners_n, reps), axis=1) - 1

    kept = jnp.arange(pno, dtype=jnp.int32)[None, :] < pair_width[:, None]
    kept = kept[:, :, None] & kept[:, None, :]
    zero = jnp.zeros((), pair_amps.dtype)
    blocks = jnp.concatenate(
        [jnp.where(kept, pair_amps, zero), jnp.where(kept, pair_exch, zero)], axis=2
    )
    rows = jnp.concatenate([jnp.maximum(asked, 0), rep[None].astype(jnp.int32)])
    sent = send_slots(rows, pair_coeff, blocks, reps)
    got = lax.all_to_all(sent, "pair", 0, 0, tiled=True)
    ready = prepare(tno_width, gap, int_left, int_right, singles, tno_energy)
    got = pltpu.with_memory_space_constraint(got, pltpu.HBM)
    far = lax.ppermute(got, "rep", [(0, 1), (1, 0)])
    far = pltpu.with_memory_space_constraint(far, pltpu.HBM)

    meta = jnp.concatenate([owners, tno_width, rep[None].astype(jnp.int32)])
    partial = triplet_energies(meta, got, far, tno_coeff, *ready, singles, tno_energy)
    energies = jnp.sum(partial, axis=(1, 2))

    shares = jnp.repeat(energies / 3.0, 3)
    shares = jnp.sum(jnp.where(at_owner, shares[None, :], 0.0), axis=1)
    shares = jnp.broadcast_to(shares[:, None], (owners_n, reps)).reshape(-1, 1)
    shares = lax.all_to_all(shares, BOTH, 0, 0, tiled=True)
    shares = jnp.sum(shares.reshape(owners_n, reps), axis=1)
    here = asked[None, :] == jnp.arange(pair_dev, dtype=jnp.int32)[:, None]
    pair_energy = jnp.sum(jnp.where(here, shares[None, :], 0.0), axis=1)
    return (energies, pair_energy)


def solution(mesh):
    both = P(BOTH)
    pair = P("pair")
    placed = (both, both, pair, pair, pair, pair, both, both, both, both, both, both)
    return jax.shard_map(
        body, mesh=mesh, in_specs=placed, out_specs=(both, pair), check_vma=False
    )
```

```python
import jax
import jax.numpy as jnp
from jax import lax
from jax.experimental import pallas as pl
from jax.experimental.pallas import tpu as pltpu
from jax.sharding import PartitionSpec as P

BOTH = ("pair", "rep")


def slots_kernel(
    rep_s, asked, coeff, blocks, out, buf, asked_v, asked_s, got, put, fetched, *, halves
):
    slots, _, lanes = out.shape
    pno = coeff.shape[1]
    dom_part = coeff.shape[2] // halves
    pieces = dom_part // lanes
    pair_rows = pno // halves
    rep = rep_s[0]
    row = lax.broadcasted_iota(jnp.int32, asked.shape, 0)
    col = lax.broadcasted_iota(jnp.int32, asked.shape, 1)
    asked_v[...] = jnp.sum(jnp.where(row == col, asked[...], 0), axis=0, keepdims=True)
    fetch = pltpu.make_async_copy(asked_v, asked_s, fetched)
    fetch.start()
    fetch.wait()

    def start(s, _):
        wanted = asked_s[0, halves * s]
        for h in range(1, halves):
            wanted = jnp.maximum(wanted, asked_s[0, halves * s + h])
        pair = jnp.maximum(wanted - 1, 0)
        for piece in range(pieces):
            pltpu.make_async_copy(
                coeff.at[pair, :, pl.ds(rep * dom_part + piece * lanes, lanes)],
                buf.at[s, pl.ds(piece * pno, pno), :],
                got.at[s],
            ).start()
        pltpu.make_async_copy(
            blocks.at[pair, pl.ds(rep * pair_rows, pair_rows), :],
            buf.at[s, pl.ds(pieces * pno, pair_rows), :],
            got.at[s],
        ).start()
        return 0

    def forward(s, _):
        pltpu.make_async_copy(out.at[s], buf.at[s], got.at[s]).wait()
        pltpu.make_async_copy(buf.at[s], out.at[s], put.at[s]).start()
        return 0

    def finish(s, _):
        pltpu.make_async_copy(buf.at[s], out.at[s], put.at[s]).wait()
        return 0

    lax.fori_loop(0, slots, start, 0)
    lax.fori_loop(0, slots, forward, 0)
    lax.fori_loop(0, slots, finish, 0)


def send_slots(rep, asked, coeff, blocks, halves):
    slots = asked.shape[0] // halves
    _, pno, domain = coeff.shape
    lanes = blocks.shape[2]
    slot_rows = pno * (domain // halves // lanes) + pno // halves
    shape = (slots, slot_rows, lanes)
    return pl.pallas_call(
        lambda *refs: slots_kernel(*refs, halves=halves),
        grid_spec=pltpu.PrefetchScalarGridSpec(
            num_scalar_prefetch=1,
            grid=(),
            in_specs=[
                pl.BlockSpec(memory_space=pltpu.VMEM),
                pl.BlockSpec(memory_space=pl.ANY),
                pl.BlockSpec(memory_space=pl.ANY),
            ],
            out_specs=pl.BlockSpec(memory_space=pl.ANY),
            scratch_shapes=[
                pltpu.VMEM(shape, jnp.bfloat16),
                pltpu.VMEM((1, asked.shape[0]), jnp.int32),
                pltpu.SMEM((1, asked.shape[0]), jnp.int32),
                pltpu.SemaphoreType.DMA((slots,)),
                pltpu.SemaphoreType.DMA((slots,)),
                pltpu.SemaphoreType.DMA(()),
            ],
        ),
        out_shape=jax.ShapeDtypeStruct(shape, jnp.bfloat16),
        name="slots",
    )(rep, asked, coeff, blocks)


def dot_nt(x, y):
    return lax.dot_general(x, y, (((1,), (1,)), ((), ())), preferred_element_type=jnp.float32)


def dot_tn(x, y):
    return lax.dot_general(x, y, (((0,), (0,)), ((), ())), preferred_element_type=jnp.float32)


def dot_tt(x, y):
    return lax.dot_general(x, y, (((0,), (1,)), ((), ())), preferred_element_type=jnp.float32)


def down_rows(row):
    size = row.shape[1]
    return jnp.transpose(jnp.broadcast_to(row, (size, size)))


STEP = 8
GROUP = 2


def prepare_kernel(widths, gap_s, left, right, singles, levels, left_t, right_t, columns):
    t = pl.program_id(0)
    size = left.shape[2]
    rows = lax.broadcasted_iota(jnp.int32, (size, size), 0)
    row_ok = rows < widths[t]
    eye = (rows == lax.broadcasted_iota(jnp.int32, (size, size), 1)).astype(jnp.float32)
    eye = eye.astype(jnp.bfloat16)
    for x in range(3):
        left_t[0, x] = jnp.where(row_ok, dot_nt(eye, left[0, x]), 0.0)
        right_t[0, x] = jnp.where(row_ok, dot_nt(eye, right[0, x]), 0.0)
    columns[0, 0] = down_rows(singles[0, 0:1, :])
    columns[0, 1] = down_rows(levels[0, 0:1, :]) + levels[0, 0:1, :] + gap_s[t]


def trip_spec(shape):
    return pl.BlockSpec((1, *shape), lambda t, *_: (t,) + (0,) * len(shape))


def prepare(widths, gap, left, right, singles, levels):
    trips, _, size, _ = left.shape
    return pl.pallas_call(
        prepare_kernel,
        grid_spec=pltpu.PrefetchScalarGridSpec(
            num_scalar_prefetch=2,
            grid=(trips,),
            in_specs=[
                trip_spec(left.shape[1:]),
                trip_spec(right.shape[1:]),
                trip_spec(singles.shape[1:]),
                trip_spec((1, size)),
            ],
            out_specs=[
                trip_spec((3, size, size)),
                trip_spec((3, size, size)),
                trip_spec((2, size, size)),
            ],
        ),
        out_shape=[
            jax.ShapeDtypeStruct((trips, 3, size, size), jnp.float32),
            jax.ShapeDtypeStruct((trips, 3, size, size), jnp.float32),
            jax.ShapeDtypeStruct((trips, 2, size, size), jnp.float32),
        ],
        compiler_params=pltpu.CompilerParams(dimension_semantics=("arbitrary",)),
        cost_estimate=pl.CostEstimate(
            flops=12 * trips * size**3, bytes_accessed=8 * trips * size**2 * 4, transcendentals=0
        ),
        name="prepare",
    )(widths, gap, left, right, singles, levels.reshape(trips, 1, size))


def energy_kernel(
    meta, levels_s, singles_s,
    own0, own1, own2, far0, far1, far2, tno, left_t, right_t, columns, singles,
    out,
    weights, exch0, exch1, exch2, connected_s, outer_s, ix,
):
    t = pl.program_id(0)
    trips = levels_s.shape[0]
    width = meta[3 * trips + t]
    rep = meta[4 * trips]
    own = (own0, own1, own2)
    far = (far0, far1, far2)
    size = tno.shape[2]
    half_dom = tno.shape[1] // 2
    lanes = own0.shape[2]
    pieces = half_dom // lanes
    pno = (own0.shape[1] * 2) // (2 * pieces + 1)
    part = pno // 2
    pairs = STEP // 2

    def stacked(refs):
        rows = []
        for ref in refs:
            cols = [ref[0, k * pno : (k + 1) * pno, :] for k in range(pieces)]
            rows.append(jnp.concatenate(cols, axis=1))
        return jnp.concatenate(rows, axis=0)

    inter = jnp.dot(
        stacked(own), tno[0, pl.ds(rep * half_dom, half_dom), :], preferred_element_type=jnp.float32
    )
    inter += jnp.dot(
        stacked(far),
        tno[0, pl.ds((1 - rep) * half_dom, half_dom), :],
        preferred_element_type=jnp.float32,
    )
    lane = lax.broadcasted_iota(jnp.int32, inter.shape, 1)
    inter = jnp.where(lane < width, inter, 0.0).astype(jnp.bfloat16)

    @pl.when(t == 0)
    def _():
        weights[...] = jnp.zeros(weights.shape, weights.dtype)

    exch = (exch0, exch1, exch2)
    spots = ((0, 256), (128, 384), (512, 640))
    for x in range(3):
        ix[x, pl.ds(rep * part, part), :] = own[x][0, pieces * pno : pieces * pno + part, :]
        ix[x, pl.ds((1 - rep) * part, part), :] = far[x][0, pieces * pno : pieces * pno + part, :]
    for x in range(3):
        inter_x = inter[x * pno : (x + 1) * pno, :]
        halfway = dot_tn(inter_x, ix[x]).astype(jnp.bfloat16)
        amps = dot_tt(inter_x, halfway[:, :pno]).astype(jnp.bfloat16)
        exch[x][...] = dot_tt(inter_x, halfway[:, pno:])
        weights[spots[x][0] : spots[x][0] + size, :size] = amps
        weights[spots[x][1] : spots[x][1] + size, size:] = amps
    single2 = singles[0, 2:3, :]

    def with_rows(m):
        def connect(side, i):
            b0 = i * STEP
            right_x = [right_t[0, x, :m, :].astype(jnp.bfloat16) for x in range(3)]
            left_x = [left_t[0, x, pl.ds(b0, STEP), :] for x in range(3)]

            def product(x, j):
                row = jnp.broadcast_to(left_x[x][j : j + 1, :], (m, size)).astype(jnp.bfloat16)
                return right_x[x] * row

            for group in range(0, pairs, GROUP):
                khatri = jnp.concatenate(
                    [
                        jnp.concatenate(
                            [
                                product(0, j), product(1, j), product(0, j + 1), product(1, j + 1),
                                product(2, j), product(2, j + 1),
                            ],
                            axis=1,
                        )
                        for j in range(2 * group, 2 * (group + GROUP), 2)
                    ],
                    axis=0,
                )
                both = jnp.dot(khatri, weights[...], preferred_element_type=jnp.float32)
                for k in range(GROUP):
                    connected_s[side, group + k, :m, :] = both[k * m : (k + 1) * m, :]
            exch2_cols = pltpu.roll(exch2[:m, :], size - b0, 1)
            for j in range(STEP):
                outer_s[side, j, :m, :] = jnp.broadcast_to(exch2_cols[:, j : j + 1], (m, size))

        def energies(side, i, total):
            b0 = i * STEP
            exch0_rows = exch0[pl.ds(b0, STEP), :]
            for j in range(STEP):
                connected = connected_s[side, j // 2, :m, (j % 2) * size : (j % 2 + 1) * size]
                complete = connected + singles_s[t, 1, b0 + j] * exch1[:m, :]
                complete += columns[0, 0, :m, :] * exch0_rows[j : j + 1, :]
                complete += outer_s[side, j, :m, :] * single2
                term = connected * complete / (columns[0, 1, :m, :] + levels_s[t, b0 + j])
                total += jnp.sum(term.reshape(m // 8, 8, size), axis=0)
            return total

        def block(i, total):
            total = energies(0, 2 * i, total)
            connect(1, 2 * i + 1)
            total = energies(1, 2 * i + 1, total)
            connect(0, 2 * i + 2)
            return total

        last = m // (2 * STEP) - 1
        connect(0, 0)
        total = lax.fori_loop(0, last, block, jnp.zeros((8, size), jnp.float32))
        total = energies(0, 2 * last, total)
        connect(1, 2 * last + 1)
        out[0] = energies(1, 2 * last + 1, total)

    needed = (width + 15) // 16 * 16
    for m in range(size // 2, size + 1, 16):
        pl.when(needed == m)(lambda m=m: with_rows(m))


def triplet_energies(meta, own, far, tno, left_t, right_t, columns, singles, levels):
    trips, _, size = tno.shape
    slot = own.shape[1:]
    pno = slot[0] * 2 // (tno.shape[1] // slot[1] + 1)

    def pair_spec(x):
        return pl.BlockSpec((1, *slot), lambda t, meta, *_: (meta[3 * t + x], 0, 0))

    return pl.pallas_call(
        energy_kernel,
        grid_spec=pltpu.PrefetchScalarGridSpec(
            num_scalar_prefetch=3,
            grid=(trips,),
            in_specs=[pair_spec(x) for x in range(3)]
            + [pair_spec(x) for x in range(3)]
            + [
                trip_spec(tno.shape[1:]),
                trip_spec(left_t.shape[1:]),
                trip_spec(right_t.shape[1:]),
                trip_spec(columns.shape[1:]),
                trip_spec(singles.shape[1:]),
            ],
            out_specs=trip_spec((8, size)),
            scratch_shapes=[
                pltpu.VMEM((6 * size, 2 * size), jnp.bfloat16),
                pltpu.VMEM((size, size), jnp.float32),
                pltpu.VMEM((size, size), jnp.float32),
                pltpu.VMEM((size, size), jnp.float32),
                pltpu.VMEM((2, STEP // 2, size, 2 * size), jnp.float32),
                pltpu.VMEM((2, STEP, size, size), jnp.float32),
                pltpu.VMEM((3, pno, 2 * pno), jnp.bfloat16),
            ],
        ),
        out_shape=jax.ShapeDtypeStruct((trips, 8, size), jnp.float32),
        compiler_params=pltpu.CompilerParams(dimension_semantics=("arbitrary",)),
        name="energy",
    )(meta, levels, singles, own, own, own, far, far, far, tno, left_t, right_t, columns, singles)


def test_entry(meta, own, far, tno, left, right, singles, levels, gap):
    trips = tno.shape[0]
    ready = prepare(meta[3 * trips : 4 * trips], gap, left, right, singles, levels)
    return jnp.sum(triplet_energies(meta, own, far, tno, *ready, singles, levels), axis=(1, 2))


def body(
    triplet_pairs, tno_width, pair_width, pair_coeff, pair_amps, pair_exch, tno_coeff,
    int_left, int_right, singles, tno_energy, gap,
):
    owners_n = lax.axis_size("pair")
    reps = lax.axis_size("rep")
    pair_dev, pno, _ = pair_coeff.shape
    rep = lax.axis_index("rep")
    references = triplet_pairs.reshape(-1)
    owners = references // pair_dev
    peers = owners_n * reps
    wide = 128
    peer = lax.broadcasted_iota(jnp.int32, (1, peers, wide), 1) // reps
    at_peer = owners[:, None, None] == peer
    wanted = jnp.sum(jnp.where(at_peer, (references % pair_dev + 1)[:, None, None], 0), axis=0)
    asked = lax.all_to_all(wanted[:, None, :], BOTH, 0, 0, tiled=True).reshape(peers, wide)

    kept = jnp.arange(pno, dtype=jnp.int32)[None, :] < pair_width[:, None]
    kept = kept[:, :, None] & kept[:, None, :]
    zero = jnp.zeros((), pair_amps.dtype)
    blocks = jnp.concatenate(
        [jnp.where(kept, pair_amps, zero), jnp.where(kept, pair_exch, zero)], axis=2
    )
    sent = send_slots(rep[None].astype(jnp.int32), asked, pair_coeff, blocks, reps)
    got = lax.all_to_all(sent, "pair", 0, 0, tiled=True)
    ready = prepare(tno_width, gap, int_left, int_right, singles, tno_energy)
    got = pltpu.with_memory_space_constraint(got, pltpu.HBM)
    far = lax.ppermute(got, "rep", [(0, 1), (1, 0)])
    far = pltpu.with_memory_space_constraint(far, pltpu.HBM)

    meta = jnp.concatenate([owners, tno_width, rep[None].astype(jnp.int32)])
    partial = triplet_energies(meta, got, far, tno_coeff, *ready, singles, tno_energy)
    energies = jnp.sum(partial, axis=(1, 2))

    shares = jnp.repeat(energies / 3.0, 3)
    shares = jnp.sum(jnp.where(at_peer, shares[:, None, None], 0.0), axis=0)
    shares = lax.all_to_all(shares[:, None, :], BOTH, 0, 0, tiled=True).reshape(peers, wide)
    here = asked == lax.broadcasted_iota(jnp.int32, (peers, wide), 1) + 1
    pair_energy = jnp.sum(jnp.where(here, shares, 0.0), axis=0)[:pair_dev]
    return (energies, pair_energy)


def solution(mesh):
    both = P(BOTH)
    pair = P("pair")
    placed = (both, both, pair, pair, pair, pair, both, both, both, both, both, both)
    return jax.shard_map(
        body, mesh=mesh, in_specs=placed, out_specs=(both, pair), check_vma=False
    )
```

```python
import jax
import jax.numpy as jnp
from jax import lax
from jax.experimental import pallas as pl
from jax.experimental.pallas import tpu as pltpu
from jax.sharding import PartitionSpec as P

BOTH = ("pair", "rep")


def slots_kernel(
    rep_s, asked, coeff, blocks, out, buf, asked_v, asked_s, got, put, fetched, *, halves
):
    slots, _, lanes = out.shape
    pno = coeff.shape[1]
    dom_part = coeff.shape[2] // halves
    pieces = dom_part // lanes
    pair_rows = pno // halves
    rep = rep_s[0]
    row = lax.broadcasted_iota(jnp.int32, asked.shape, 0)
    col = lax.broadcasted_iota(jnp.int32, asked.shape, 1)
    asked_v[...] = jnp.sum(jnp.where(row == col, asked[...], 0), axis=0, keepdims=True)
    fetch = pltpu.make_async_copy(asked_v, asked_s, fetched)
    fetch.start()
    fetch.wait()

    def start(s, _):
        wanted = asked_s[0, halves * s]
        for h in range(1, halves):
            wanted = jnp.maximum(wanted, asked_s[0, halves * s + h])
        pair = jnp.maximum(wanted - 1, 0)
        for piece in range(pieces):
            pltpu.make_async_copy(
                coeff.at[pair, :, pl.ds(rep * dom_part + piece * lanes, lanes)],
                buf.at[s, pl.ds(piece * pno, pno), :],
                got.at[s],
            ).start()
        pltpu.make_async_copy(
            blocks.at[pair, pl.ds(rep * pair_rows, pair_rows), :],
            buf.at[s, pl.ds(pieces * pno, pair_rows), :],
            got.at[s],
        ).start()
        return 0

    def forward(s, _):
        pltpu.make_async_copy(out.at[s], buf.at[s], got.at[s]).wait()
        pltpu.make_async_copy(buf.at[s], out.at[s], put.at[s]).start()
        return 0

    def finish(s, _):
        pltpu.make_async_copy(buf.at[s], out.at[s], put.at[s]).wait()
        return 0

    lax.fori_loop(0, slots, start, 0)
    lax.fori_loop(0, slots, forward, 0)
    lax.fori_loop(0, slots, finish, 0)


def send_slots(rep, asked, coeff, blocks, halves):
    slots = asked.shape[0] // halves
    _, pno, domain = coeff.shape
    lanes = blocks.shape[2]
    slot_rows = pno * (domain // halves // lanes) + pno // halves
    shape = (slots, slot_rows, lanes)
    return pl.pallas_call(
        lambda *refs: slots_kernel(*refs, halves=halves),
        grid_spec=pltpu.PrefetchScalarGridSpec(
            num_scalar_prefetch=1,
            grid=(),
            in_specs=[
                pl.BlockSpec(memory_space=pltpu.VMEM),
                pl.BlockSpec(memory_space=pl.ANY),
                pl.BlockSpec(memory_space=pl.ANY),
            ],
            out_specs=pl.BlockSpec(memory_space=pl.ANY),
            scratch_shapes=[
                pltpu.VMEM(shape, jnp.bfloat16),
                pltpu.VMEM((1, asked.shape[0]), jnp.int32),
                pltpu.SMEM((1, asked.shape[0]), jnp.int32),
                pltpu.SemaphoreType.DMA((slots,)),
                pltpu.SemaphoreType.DMA((slots,)),
                pltpu.SemaphoreType.DMA(()),
            ],
        ),
        out_shape=jax.ShapeDtypeStruct(shape, jnp.bfloat16),
        name="slots",
    )(rep, asked, coeff, blocks)


def dot_nt(x, y):
    return lax.dot_general(x, y, (((1,), (1,)), ((), ())), preferred_element_type=jnp.float32)


def dot_tn(x, y):
    return lax.dot_general(x, y, (((0,), (0,)), ((), ())), preferred_element_type=jnp.float32)


def dot_tt(x, y):
    return lax.dot_general(x, y, (((0,), (1,)), ((), ())), preferred_element_type=jnp.float32)


def down_rows(row):
    size = row.shape[1]
    return jnp.transpose(jnp.broadcast_to(row, (size, size)))


STEP = 8
GROUP = 2


def prepare_kernel(widths, gap_s, left, right, singles, levels, left_t, right_t, columns):
    t = pl.program_id(0)
    size = left.shape[2]
    rows = lax.broadcasted_iota(jnp.int32, (size, size), 0)
    row_ok = rows < widths[t]
    eye = (rows == lax.broadcasted_iota(jnp.int32, (size, size), 1)).astype(jnp.float32)
    eye = eye.astype(jnp.bfloat16)
    for x in range(3):
        left_t[0, x] = jnp.where(row_ok, dot_nt(eye, left[0, x]), 0.0)
        right_t[0, x] = jnp.where(row_ok, dot_nt(eye, right[0, x]), 0.0)
    columns[0, 0] = down_rows(singles[0, 0:1, :])
    columns[0, 1] = down_rows(levels[0, 0:1, :]) + levels[0, 0:1, :] + gap_s[t]


def trip_spec(shape):
    return pl.BlockSpec((1, *shape), lambda t, *_: (t,) + (0,) * len(shape))


def prepare(widths, gap, left, right, singles, levels):
    trips, _, size, _ = left.shape
    return pl.pallas_call(
        prepare_kernel,
        grid_spec=pltpu.PrefetchScalarGridSpec(
            num_scalar_prefetch=2,
            grid=(trips,),
            in_specs=[
                trip_spec(left.shape[1:]),
                trip_spec(right.shape[1:]),
                trip_spec(singles.shape[1:]),
                trip_spec((1, size)),
            ],
            out_specs=[
                trip_spec((3, size, size)),
                trip_spec((3, size, size)),
                trip_spec((2, size, size)),
            ],
        ),
        out_shape=[
            jax.ShapeDtypeStruct((trips, 3, size, size), jnp.float32),
            jax.ShapeDtypeStruct((trips, 3, size, size), jnp.float32),
            jax.ShapeDtypeStruct((trips, 2, size, size), jnp.float32),
        ],
        compiler_params=pltpu.CompilerParams(dimension_semantics=("arbitrary",)),
        cost_estimate=pl.CostEstimate(
            flops=12 * trips * size**3, bytes_accessed=8 * trips * size**2 * 4, transcendentals=0
        ),
        name="prepare",
    )(widths, gap, left, right, singles, levels.reshape(trips, 1, size))


def energy_kernel(
    meta, levels_s, singles_s,
    own0, own1, own2, far0, far1, far2, tno, left_t, right_t, columns, singles,
    out,
    weights, exch0, exch1, exch2, connected_s, outer_s, ix,
):
    t = pl.program_id(0)
    trips = levels_s.shape[0]
    width = meta[3 * trips + t]
    rep = meta[4 * trips]
    own = (own0, own1, own2)
    far = (far0, far1, far2)
    size = tno.shape[2]
    half_dom = tno.shape[1] // 2
    lanes = own0.shape[2]
    pieces = half_dom // lanes
    pno = (own0.shape[1] * 2) // (2 * pieces + 1)
    part = pno // 2
    pairs = STEP // 2

    def stacked(refs):
        rows = []
        for ref in refs:
            cols = [ref[0, k * pno : (k + 1) * pno, :] for k in range(pieces)]
            rows.append(jnp.concatenate(cols, axis=1))
        return jnp.concatenate(rows, axis=0)

    inter = jnp.dot(
        stacked(own), tno[0, pl.ds(rep * half_dom, half_dom), :], preferred_element_type=jnp.float32
    )
    inter += jnp.dot(
        stacked(far),
        tno[0, pl.ds((1 - rep) * half_dom, half_dom), :],
        preferred_element_type=jnp.float32,
    )
    lane = lax.broadcasted_iota(jnp.int32, inter.shape, 1)
    inter = jnp.where(lane < width, inter, 0.0).astype(jnp.bfloat16)

    @pl.when(t == 0)
    def _():
        weights[...] = jnp.zeros(weights.shape, weights.dtype)

    exch = (exch0, exch1, exch2)
    spots = ((0, 256), (128, 384), (512, 640))
    for x in range(3):
        ix[x, pl.ds(rep * part, part), :] = own[x][0, pieces * pno : pieces * pno + part, :]
        ix[x, pl.ds((1 - rep) * part, part), :] = far[x][0, pieces * pno : pieces * pno + part, :]
    for x in range(3):
        inter_x = inter[x * pno : (x + 1) * pno, :]
        halfway = dot_tn(inter_x, ix[x]).astype(jnp.bfloat16)
        amps = dot_tt(inter_x, halfway[:, :pno]).astype(jnp.bfloat16)
        exch[x][...] = dot_tt(inter_x, halfway[:, pno:])
        weights[spots[x][0] : spots[x][0] + size, :size] = amps
        weights[spots[x][1] : spots[x][1] + size, size:] = amps
    single2 = singles[0, 2:3, :]

    def with_rows(m):
        def connect(side, i):
            b0 = i * STEP
            right_x = [right_t[0, x, :m, :].astype(jnp.bfloat16) for x in range(3)]
            left_x = [left_t[0, x, pl.ds(b0, STEP), :] for x in range(3)]

            def product(x, j):
                row = jnp.broadcast_to(left_x[x][j : j + 1, :], (m, size)).astype(jnp.bfloat16)
                return right_x[x] * row

            for group in range(0, pairs, GROUP):
                khatri = jnp.concatenate(
                    [
                        jnp.concatenate(
                            [
                                product(0, j), product(1, j), product(0, j + 1), product(1, j + 1),
                                product(2, j), product(2, j + 1),
                            ],
                            axis=1,
                        )
                        for j in range(2 * group, 2 * (group + GROUP), 2)
                    ],
                    axis=0,
                )
                both = jnp.dot(khatri, weights[...], preferred_element_type=jnp.float32)
                for k in range(GROUP):
                    connected_s[side, group + k, :m, :] = both[k * m : (k + 1) * m, :]
            for j in range(STEP):
                outer_s[side, j, :m, :] = jnp.broadcast_to(exch2[:m, b0 + j : b0 + j + 1], (m, size))

        def energies(side, i, total):
            b0 = i * STEP
            exch0_rows = exch0[pl.ds(b0, STEP), :]
            for j in range(STEP):
                connected = connected_s[side, j // 2, :m, (j % 2) * size : (j % 2 + 1) * size]
                complete = connected + singles_s[t, 1, b0 + j] * exch1[:m, :]
                complete += columns[0, 0, :m, :] * exch0_rows[j : j + 1, :]
                complete += outer_s[side, j, :m, :] * single2
                term = connected * complete / (columns[0, 1, :m, :] + levels_s[t, b0 + j])
                total += jnp.sum(term.reshape(m // 8, 8, size), axis=0)
            return total

        steps = m // STEP
        total = jnp.zeros((8, size), jnp.float32)
        connect(0, 0)
        for i in range(steps):
            total = energies(i % 2, i, total)
            if i + 1 < steps:
                connect((i + 1) % 2, i + 1)
        out[0] = total

    needed = (width + 15) // 16 * 16
    for m in range(size // 2, size + 1, 16):
        pl.when(needed == m)(lambda m=m: with_rows(m))


def triplet_energies(meta, own, far, tno, left_t, right_t, columns, singles, levels):
    trips, _, size = tno.shape
    slot = own.shape[1:]
    pno = slot[0] * 2 // (tno.shape[1] // slot[1] + 1)

    def pair_spec(x):
        return pl.BlockSpec((1, *slot), lambda t, meta, *_: (meta[3 * t + x], 0, 0))

    return pl.pallas_call(
        energy_kernel,
        grid_spec=pltpu.PrefetchScalarGridSpec(
            num_scalar_prefetch=3,
            grid=(trips,),
            in_specs=[pair_spec(x) for x in range(3)]
            + [pair_spec(x) for x in range(3)]
            + [
                trip_spec(tno.shape[1:]),
                trip_spec(left_t.shape[1:]),
                trip_spec(right_t.shape[1:]),
                trip_spec(columns.shape[1:]),
                trip_spec(singles.shape[1:]),
            ],
            out_specs=trip_spec((8, size)),
            scratch_shapes=[
                pltpu.VMEM((6 * size, 2 * size), jnp.bfloat16),
                pltpu.VMEM((size, size), jnp.float32),
                pltpu.VMEM((size, size), jnp.float32),
                pltpu.VMEM((size, size), jnp.float32),
                pltpu.VMEM((2, STEP // 2, size, 2 * size), jnp.float32),
                pltpu.VMEM((2, STEP, size, size), jnp.float32),
                pltpu.VMEM((3, pno, 2 * pno), jnp.bfloat16),
            ],
        ),
        out_shape=jax.ShapeDtypeStruct((trips, 8, size), jnp.float32),
        compiler_params=pltpu.CompilerParams(dimension_semantics=("arbitrary",)),
        name="energy",
    )(meta, levels, singles, own, own, own, far, far, far, tno, left_t, right_t, columns, singles)


def test_entry(meta, own, far, tno, left, right, singles, levels, gap):
    trips = tno.shape[0]
    ready = prepare(meta[3 * trips : 4 * trips], gap, left, right, singles, levels)
    return jnp.sum(triplet_energies(meta, own, far, tno, *ready, singles, levels), axis=(1, 2))


def body(
    triplet_pairs, tno_width, pair_width, pair_coeff, pair_amps, pair_exch, tno_coeff,
    int_left, int_right, singles, tno_energy, gap,
):
    owners_n = lax.axis_size("pair")
    reps = lax.axis_size("rep")
    pair_dev, pno, _ = pair_coeff.shape
    rep = lax.axis_index("rep")
    references = triplet_pairs.reshape(-1)
    owners = references // pair_dev
    peers = owners_n * reps
    wide = 128
    peer = lax.broadcasted_iota(jnp.int32, (1, peers, wide), 1) // reps
    at_peer = owners[:, None, None] == peer
    wanted = jnp.sum(jnp.where(at_peer, (references % pair_dev + 1)[:, None, None], 0), axis=0)
    asked = lax.all_to_all(wanted[:, None, :], BOTH, 0, 0, tiled=True).reshape(peers, wide)

    kept = jnp.arange(pno, dtype=jnp.int32)[None, :] < pair_width[:, None]
    kept = kept[:, :, None] & kept[:, None, :]
    zero = jnp.zeros((), pair_amps.dtype)
    blocks = jnp.concatenate(
        [jnp.where(kept, pair_amps, zero), jnp.where(kept, pair_exch, zero)], axis=2
    )
    sent = send_slots(rep[None].astype(jnp.int32), asked, pair_coeff, blocks, reps)
    got = lax.all_to_all(sent, "pair", 0, 0, tiled=True)
    ready = prepare(tno_width, gap, int_left, int_right, singles, tno_energy)
    got = pltpu.with_memory_space_constraint(got, pltpu.HBM)
    far = lax.ppermute(got, "rep", [(0, 1), (1, 0)])
    far = pltpu.with_memory_space_constraint(far, pltpu.HBM)

    meta = jnp.concatenate([owners, tno_width, rep[None].astype(jnp.int32)])
    partial = triplet_energies(meta, got, far, tno_coeff, *ready, singles, tno_energy)
    energies = jnp.sum(partial, axis=(1, 2))

    shares = jnp.repeat(energies / 3.0, 3)
    shares = jnp.sum(jnp.where(at_peer, shares[:, None, None], 0.0), axis=0)
    shares = lax.all_to_all(shares[:, None, :], BOTH, 0, 0, tiled=True).reshape(peers, wide)
    here = asked == lax.broadcasted_iota(jnp.int32, (peers, wide), 1) + 1
    pair_energy = jnp.sum(jnp.where(here, shares, 0.0), axis=0)[:pair_dev]
    return (energies, pair_energy)


def solution(mesh):
    both = P(BOTH)
    pair = P("pair")
    placed = (both, both, pair, pair, pair, pair, both, both, both, both, both, both)
    return jax.shard_map(
        body, mesh=mesh, in_specs=placed, out_specs=(both, pair), check_vma=False
    )
```

```python
import jax
import jax.numpy as jnp
from jax import lax
from jax.experimental import pallas as pl
from jax.experimental.pallas import tpu as pltpu
from jax.sharding import PartitionSpec as P

BOTH = ("pair", "rep")


def slots_kernel(
    rep_s, asked, coeff, blocks, out, buf, asked_v, asked_s, got, put, fetched, *, halves
):
    slots, _, lanes = out.shape
    pno = coeff.shape[1]
    dom_part = coeff.shape[2] // halves
    pieces = dom_part // lanes
    pair_rows = pno // halves
    rep = rep_s[0]
    row = lax.broadcasted_iota(jnp.int32, asked.shape, 0)
    col = lax.broadcasted_iota(jnp.int32, asked.shape, 1)
    asked_v[...] = jnp.sum(jnp.where(row == col, asked[...], 0), axis=0, keepdims=True)
    fetch = pltpu.make_async_copy(asked_v, asked_s, fetched)
    fetch.start()
    fetch.wait()

    def start(s, _):
        wanted = asked_s[0, halves * s]
        for h in range(1, halves):
            wanted = jnp.maximum(wanted, asked_s[0, halves * s + h])
        pair = jnp.maximum(wanted - 1, 0)
        for piece in range(pieces):
            pltpu.make_async_copy(
                coeff.at[pair, :, pl.ds(rep * dom_part + piece * lanes, lanes)],
                buf.at[s, pl.ds(piece * pno, pno), :],
                got.at[s],
            ).start()
        pltpu.make_async_copy(
            blocks.at[pair, pl.ds(rep * pair_rows, pair_rows), :],
            buf.at[s, pl.ds(pieces * pno, pair_rows), :],
            got.at[s],
        ).start()
        return 0

    def forward(s, _):
        pltpu.make_async_copy(out.at[s], buf.at[s], got.at[s]).wait()
        pltpu.make_async_copy(buf.at[s], out.at[s], put.at[s]).start()
        return 0

    def finish(s, _):
        pltpu.make_async_copy(buf.at[s], out.at[s], put.at[s]).wait()
        return 0

    lax.fori_loop(0, slots, start, 0)
    lax.fori_loop(0, slots, forward, 0)
    lax.fori_loop(0, slots, finish, 0)


def send_slots(rep, asked, coeff, blocks, halves):
    slots = asked.shape[0] // halves
    _, pno, domain = coeff.shape
    lanes = blocks.shape[2]
    slot_rows = pno * (domain // halves // lanes) + pno // halves
    shape = (slots, slot_rows, lanes)
    return pl.pallas_call(
        lambda *refs: slots_kernel(*refs, halves=halves),
        grid_spec=pltpu.PrefetchScalarGridSpec(
            num_scalar_prefetch=1,
            grid=(),
            in_specs=[
                pl.BlockSpec(memory_space=pltpu.VMEM),
                pl.BlockSpec(memory_space=pl.ANY),
                pl.BlockSpec(memory_space=pl.ANY),
            ],
            out_specs=pl.BlockSpec(memory_space=pl.ANY),
            scratch_shapes=[
                pltpu.VMEM(shape, jnp.bfloat16),
                pltpu.VMEM((1, asked.shape[0]), jnp.int32),
                pltpu.SMEM((1, asked.shape[0]), jnp.int32),
                pltpu.SemaphoreType.DMA((slots,)),
                pltpu.SemaphoreType.DMA((slots,)),
                pltpu.SemaphoreType.DMA(()),
            ],
        ),
        out_shape=jax.ShapeDtypeStruct(shape, jnp.bfloat16),
        name="slots",
    )(rep, asked, coeff, blocks)


def dot_nt(x, y):
    return lax.dot_general(x, y, (((1,), (1,)), ((), ())), preferred_element_type=jnp.float32)


def dot_tn(x, y):
    return lax.dot_general(x, y, (((0,), (0,)), ((), ())), preferred_element_type=jnp.float32)


def dot_tt(x, y):
    return lax.dot_general(x, y, (((0,), (1,)), ((), ())), preferred_element_type=jnp.float32)


def down_rows(row):
    size = row.shape[1]
    return jnp.transpose(jnp.broadcast_to(row, (size, size)))


STEP = 8
GROUP = 2


def prepare_kernel(widths, gap_s, left, right, singles, levels, left_t, right_t, columns):
    t = pl.program_id(0)
    size = left.shape[2]
    rows = lax.broadcasted_iota(jnp.int32, (size, size), 0)
    row_ok = rows < widths[t]
    eye = (rows == lax.broadcasted_iota(jnp.int32, (size, size), 1)).astype(jnp.float32)
    eye = eye.astype(jnp.bfloat16)
    for x in range(3):
        left_t[0, x] = jnp.where(row_ok, dot_nt(eye, left[0, x]), 0.0)
        right_t[0, x] = jnp.where(row_ok, dot_nt(eye, right[0, x]), 0.0)
    columns[0, 0] = down_rows(singles[0, 0:1, :])
    columns[0, 1] = down_rows(levels[0, 0:1, :]) + levels[0, 0:1, :] + gap_s[t]


def trip_spec(shape):
    return pl.BlockSpec((1, *shape), lambda t, *_: (t,) + (0,) * len(shape))


def prepare(widths, gap, left, right, singles, levels):
    trips, _, size, _ = left.shape
    return pl.pallas_call(
        prepare_kernel,
        grid_spec=pltpu.PrefetchScalarGridSpec(
            num_scalar_prefetch=2,
            grid=(trips,),
            in_specs=[
                trip_spec(left.shape[1:]),
                trip_spec(right.shape[1:]),
                trip_spec(singles.shape[1:]),
                trip_spec((1, size)),
            ],
            out_specs=[
                trip_spec((3, size, size)),
                trip_spec((3, size, size)),
                trip_spec((2, size, size)),
            ],
        ),
        out_shape=[
            jax.ShapeDtypeStruct((trips, 3, size, size), jnp.float32),
            jax.ShapeDtypeStruct((trips, 3, size, size), jnp.float32),
            jax.ShapeDtypeStruct((trips, 2, size, size), jnp.float32),
        ],
        compiler_params=pltpu.CompilerParams(dimension_semantics=("arbitrary",)),
        cost_estimate=pl.CostEstimate(
            flops=12 * trips * size**3, bytes_accessed=8 * trips * size**2 * 4, transcendentals=0
        ),
        name="prepare",
    )(widths, gap, left, right, singles, levels.reshape(trips, 1, size))


def energy_kernel(
    meta, levels_s, singles_s,
    own0, own1, own2, far0, far1, far2, tno, left_t, right_t, columns, singles,
    out,
    weights, exch, next_weights, next_exch, connected_s, outer_s, ix,
):
    step = pl.program_id(0)
    trips = levels_s.shape[0]
    t = jnp.maximum(step - 1, 0)
    width = meta[3 * trips + t]
    next_width = meta[3 * trips + jnp.minimum(step, trips - 1)]
    rep = meta[4 * trips]
    own = (own0, own1, own2)
    far = (far0, far1, far2)
    size = tno.shape[2]
    half_dom = tno.shape[1] // 2
    lanes = own0.shape[2]
    pieces = half_dom // lanes
    pno = (own0.shape[1] * 2) // (2 * pieces + 1)
    part = pno // 2
    pairs = STEP // 2

    def stacked(refs):
        rows = []
        for ref in refs:
            cols = [ref[0, k * pno : (k + 1) * pno, :] for k in range(pieces)]
            rows.append(jnp.concatenate(cols, axis=1))
        return jnp.concatenate(rows, axis=0)

    def project():
        inter = jnp.dot(
            stacked(own),
            tno[0, pl.ds(rep * half_dom, half_dom), :],
            preferred_element_type=jnp.float32,
        )
        inter += jnp.dot(
            stacked(far),
            tno[0, pl.ds((1 - rep) * half_dom, half_dom), :],
            preferred_element_type=jnp.float32,
        )
        lane = lax.broadcasted_iota(jnp.int32, inter.shape, 1)
        inter = jnp.where(lane < next_width, inter, 0.0).astype(jnp.bfloat16)
        for x in range(3):
            mine = own[x][0, pieces * pno : pieces * pno + part, :]
            other = far[x][0, pieces * pno : pieces * pno + part, :]
            ix[x, pl.ds(rep * part, part), :] = mine
            ix[x, pl.ds((1 - rep) * part, part), :] = other
        for x in range(3):
            inter_x = inter[x * pno : (x + 1) * pno, :]
            halfway = dot_tn(inter_x, ix[x]).astype(jnp.bfloat16)
            next_weights[x] = dot_tt(inter_x, halfway[:, :pno]).astype(jnp.bfloat16)
            next_exch[x] = dot_tt(inter_x, halfway[:, pno:])

    single2 = singles[0, 2:3, :]
    spots = ((0, 256), (128, 384), (512, 640))

    def with_rows(m):
        def connect(side, i):
            b0 = i * STEP
            right_x = [right_t[0, x, :m, :].astype(jnp.bfloat16) for x in range(3)]
            left_x = [left_t[0, x, pl.ds(b0, STEP), :] for x in range(3)]

            def product(x, j):
                row = jnp.broadcast_to(left_x[x][j : j + 1, :], (m, size)).astype(jnp.bfloat16)
                return right_x[x] * row

            for group in range(0, pairs, GROUP):
                khatri = jnp.concatenate(
                    [
                        jnp.concatenate(
                            [
                                product(0, j), product(1, j), product(0, j + 1), product(1, j + 1),
                                product(2, j), product(2, j + 1),
                            ],
                            axis=1,
                        )
                        for j in range(2 * group, 2 * (group + GROUP), 2)
                    ],
                    axis=0,
                )
                both = jnp.dot(khatri, weights[...], preferred_element_type=jnp.float32)
                for k in range(GROUP):
                    connected_s[side, group + k, :m, :] = both[k * m : (k + 1) * m, :]
            for j in range(STEP):
                column = exch[2, :m, b0 + j : b0 + j + 1]
                outer_s[side, j, :m, :] = jnp.broadcast_to(column, (m, size))

        def energies(side, i, total):
            b0 = i * STEP
            exch0_rows = exch[0, pl.ds(b0, STEP), :]
            for j in range(STEP):
                connected = connected_s[side, j // 2, :m, (j % 2) * size : (j % 2 + 1) * size]
                complete = connected + singles_s[t, 1, b0 + j] * exch[1, :m, :]
                complete += columns[0, 0, :m, :] * exch0_rows[j : j + 1, :]
                complete += outer_s[side, j, :m, :] * single2
                term = connected * complete / (columns[0, 1, :m, :] + levels_s[t, b0 + j])
                total += jnp.sum(term.reshape(m // 8, 8, size), axis=0)
            return total

        steps = m // STEP
        total = jnp.zeros((8, size), jnp.float32)
        connect(0, 0)
        for i in range(steps):
            total = energies(i % 2, i, total)
            if i + 1 < steps:
                connect((i + 1) % 2, i + 1)
            if i == 1:
                project()
        out[0] = total

    @pl.when(step == 0)
    def _():
        weights[...] = jnp.zeros(weights.shape, weights.dtype)
        project()

    @pl.when(step > 0)
    def _():
        for x in range(3):
            amps = next_weights[x]
            weights[spots[x][0] : spots[x][0] + size, :size] = amps
            weights[spots[x][1] : spots[x][1] + size, size:] = amps
            exch[x] = next_exch[x]
        needed = (width + 15) // 16 * 16
        for m in range(size // 2, size + 1, 16):
            pl.when(needed == m)(lambda m=m: with_rows(m))


def triplet_energies(meta, own, far, tno, left_t, right_t, columns, singles, levels):
    trips, _, size = tno.shape
    slot = own.shape[1:]
    pno = slot[0] * 2 // (tno.shape[1] // slot[1] + 1)

    def ahead(s):
        return jnp.minimum(s, trips - 1)

    def behind_spec(shape):
        return pl.BlockSpec(
            (1, *shape), lambda s, *_: (jnp.maximum(s - 1, 0),) + (0,) * len(shape)
        )

    def pair_spec(x):
        return pl.BlockSpec((1, *slot), lambda s, meta, *_: (meta[3 * ahead(s) + x], 0, 0))

    return pl.pallas_call(
        energy_kernel,
        grid_spec=pltpu.PrefetchScalarGridSpec(
            num_scalar_prefetch=3,
            grid=(trips + 1,),
            in_specs=[pair_spec(x) for x in range(3)]
            + [pair_spec(x) for x in range(3)]
            + [
                pl.BlockSpec((1, *tno.shape[1:]), lambda s, *_: (ahead(s), 0, 0)),
                behind_spec(left_t.shape[1:]),
                behind_spec(right_t.shape[1:]),
                behind_spec(columns.shape[1:]),
                behind_spec(singles.shape[1:]),
            ],
            out_specs=behind_spec((8, size)),
            scratch_shapes=[
                pltpu.VMEM((6 * size, 2 * size), jnp.bfloat16),
                pltpu.VMEM((3, size, size), jnp.float32),
                pltpu.VMEM((3, size, size), jnp.bfloat16),
                pltpu.VMEM((3, size, size), jnp.float32),
                pltpu.VMEM((2, STEP // 2, size, 2 * size), jnp.float32),
                pltpu.VMEM((2, STEP, size, size), jnp.float32),
                pltpu.VMEM((3, pno, 2 * pno), jnp.bfloat16),
            ],
        ),
        out_shape=jax.ShapeDtypeStruct((trips, 8, size), jnp.float32),
        compiler_params=pltpu.CompilerParams(dimension_semantics=("arbitrary",)),
        name="energy",
    )(meta, levels, singles, own, own, own, far, far, far, tno, left_t, right_t, columns, singles)


def test_entry(meta, own, far, tno, left, right, singles, levels, gap):
    trips = tno.shape[0]
    ready = prepare(meta[3 * trips : 4 * trips], gap, left, right, singles, levels)
    return jnp.sum(triplet_energies(meta, own, far, tno, *ready, singles, levels), axis=(1, 2))


def body(
    triplet_pairs, tno_width, pair_width, pair_coeff, pair_amps, pair_exch, tno_coeff,
    int_left, int_right, singles, tno_energy, gap,
):
    owners_n = lax.axis_size("pair")
    reps = lax.axis_size("rep")
    pair_dev, pno, _ = pair_coeff.shape
    rep = lax.axis_index("rep")
    references = triplet_pairs.reshape(-1)
    owners = references // pair_dev
    peers = owners_n * reps
    wide = 128
    peer = lax.broadcasted_iota(jnp.int32, (1, peers, wide), 1) // reps
    at_peer = owners[:, None, None] == peer
    wanted = jnp.sum(jnp.where(at_peer, (references % pair_dev + 1)[:, None, None], 0), axis=0)
    asked = lax.all_to_all(wanted[:, None, :], BOTH, 0, 0, tiled=True).reshape(peers, wide)

    kept = jnp.arange(pno, dtype=jnp.int32)[None, :] < pair_width[:, None]
    kept = kept[:, :, None] & kept[:, None, :]
    zero = jnp.zeros((), pair_amps.dtype)
    blocks = jnp.concatenate(
        [jnp.where(kept, pair_amps, zero), jnp.where(kept, pair_exch, zero)], axis=2
    )
    sent = send_slots(rep[None].astype(jnp.int32), asked, pair_coeff, blocks, reps)
    got = lax.all_to_all(sent, "pair", 0, 0, tiled=True)
    ready = prepare(tno_width, gap, int_left, int_right, singles, tno_energy)
    got, ready = lax.optimization_barrier((got, ready))
    got = pltpu.with_memory_space_constraint(got, pltpu.HBM)
    far = lax.ppermute(got, "rep", [(0, 1), (1, 0)])
    far = pltpu.with_memory_space_constraint(far, pltpu.HBM)

    meta = jnp.concatenate([owners, tno_width, rep[None].astype(jnp.int32)])
    partial = triplet_energies(meta, got, far, tno_coeff, *ready, singles, tno_energy)
    energies = jnp.sum(partial, axis=(1, 2))

    shares = jnp.repeat(energies / 3.0, 3)
    shares = jnp.sum(jnp.where(at_peer, shares[:, None, None], 0.0), axis=0)
    shares = lax.all_to_all(shares[:, None, :], BOTH, 0, 0, tiled=True).reshape(peers, wide)
    here = asked == lax.broadcasted_iota(jnp.int32, (peers, wide), 1) + 1
    pair_energy = jnp.sum(jnp.where(here, shares, 0.0), axis=0)[:pair_dev]
    return (energies, pair_energy)


def solution(mesh):
    both = P(BOTH)
    pair = P("pair")
    placed = (both, both, pair, pair, pair, pair, both, both, both, both, both, both)
    return jax.shard_map(
        body, mesh=mesh, in_specs=placed, out_specs=(both, pair), check_vma=False
    )
```

```python
import jax
import jax.numpy as jnp
from jax import lax
from jax.experimental import pallas as pl
from jax.experimental.pallas import tpu as pltpu
from jax.sharding import PartitionSpec as P

BOTH = ("pair", "rep")


def slots_kernel(
    rep_s, asked, coeff, blocks, out, buf, asked_v, asked_s, got, put, fetched, *, halves
):
    slots, _, lanes = out.shape
    pno = coeff.shape[1]
    dom_part = coeff.shape[2] // halves
    pieces = dom_part // lanes
    pair_rows = pno // halves
    rep = rep_s[0]
    row = lax.broadcasted_iota(jnp.int32, asked.shape, 0)
    col = lax.broadcasted_iota(jnp.int32, asked.shape, 1)
    asked_v[...] = jnp.sum(jnp.where(row == col, asked[...], 0), axis=0, keepdims=True)
    fetch = pltpu.make_async_copy(asked_v, asked_s, fetched)
    fetch.start()
    fetch.wait()

    def start(s, _):
        wanted = asked_s[0, halves * s]
        for h in range(1, halves):
            wanted = jnp.maximum(wanted, asked_s[0, halves * s + h])
        pair = jnp.maximum(wanted - 1, 0)
        for piece in range(pieces):
            pltpu.make_async_copy(
                coeff.at[pair, :, pl.ds(rep * dom_part + piece * lanes, lanes)],
                buf.at[s, pl.ds(piece * pno, pno), :],
                got.at[s],
            ).start()
        pltpu.make_async_copy(
            blocks.at[pair, pl.ds(rep * pair_rows, pair_rows), :],
            buf.at[s, pl.ds(pieces * pno, pair_rows), :],
            got.at[s],
        ).start()
        return 0

    def forward(s, _):
        pltpu.make_async_copy(out.at[s], buf.at[s], got.at[s]).wait()
        pltpu.make_async_copy(buf.at[s], out.at[s], put.at[s]).start()
        return 0

    def finish(s, _):
        pltpu.make_async_copy(buf.at[s], out.at[s], put.at[s]).wait()
        return 0

    lax.fori_loop(0, slots, start, 0)
    lax.fori_loop(0, slots, forward, 0)
    lax.fori_loop(0, slots, finish, 0)


def send_slots(rep, asked, coeff, blocks, halves):
    slots = asked.shape[0] // halves
    _, pno, domain = coeff.shape
    lanes = blocks.shape[2]
    slot_rows = pno * (domain // halves // lanes) + pno // halves
    shape = (slots, slot_rows, lanes)
    return pl.pallas_call(
        lambda *refs: slots_kernel(*refs, halves=halves),
        grid_spec=pltpu.PrefetchScalarGridSpec(
            num_scalar_prefetch=1,
            grid=(),
            in_specs=[
                pl.BlockSpec(memory_space=pltpu.VMEM),
                pl.BlockSpec(memory_space=pl.ANY),
                pl.BlockSpec(memory_space=pl.ANY),
            ],
            out_specs=pl.BlockSpec(memory_space=pl.ANY),
            scratch_shapes=[
                pltpu.VMEM(shape, jnp.bfloat16),
                pltpu.VMEM((1, asked.shape[0]), jnp.int32),
                pltpu.SMEM((1, asked.shape[0]), jnp.int32),
                pltpu.SemaphoreType.DMA((slots,)),
                pltpu.SemaphoreType.DMA((slots,)),
                pltpu.SemaphoreType.DMA(()),
            ],
        ),
        out_shape=jax.ShapeDtypeStruct(shape, jnp.bfloat16),
        name="slots",
    )(rep, asked, coeff, blocks)


def dot_nt(x, y):
    return lax.dot_general(x, y, (((1,), (1,)), ((), ())), preferred_element_type=jnp.float32)


def dot_tn(x, y):
    return lax.dot_general(x, y, (((0,), (0,)), ((), ())), preferred_element_type=jnp.float32)


def dot_tt(x, y):
    return lax.dot_general(x, y, (((0,), (1,)), ((), ())), preferred_element_type=jnp.float32)


def down_rows(row):
    size = row.shape[1]
    return jnp.transpose(jnp.broadcast_to(row, (size, size)))


STEP = 8
GROUP = 2


def prepare_kernel(widths, gap_s, left, right, singles, levels, left_t, right_t, columns):
    t = pl.program_id(0)
    size = left.shape[2]
    rows = lax.broadcasted_iota(jnp.int32, (size, size), 0)
    row_ok = rows < widths[t]
    eye = (rows == lax.broadcasted_iota(jnp.int32, (size, size), 1)).astype(jnp.float32)
    eye = eye.astype(jnp.bfloat16)
    for x in range(3):
        left_t[0, x] = jnp.where(row_ok, dot_nt(eye, left[0, x]), 0.0)
        right_t[0, x] = jnp.where(row_ok, dot_nt(eye, right[0, x]), 0.0)
    columns[0, 0] = down_rows(singles[0, 0:1, :])
    columns[0, 1] = down_rows(levels[0, 0:1, :]) + levels[0, 0:1, :] + gap_s[t]


def trip_spec(shape):
    return pl.BlockSpec((1, *shape), lambda t, *_: (t,) + (0,) * len(shape))


def prepare(widths, gap, left, right, singles, levels):
    trips, _, size, _ = left.shape
    return pl.pallas_call(
        prepare_kernel,
        grid_spec=pltpu.PrefetchScalarGridSpec(
            num_scalar_prefetch=2,
            grid=(trips,),
            in_specs=[
                trip_spec(left.shape[1:]),
                trip_spec(right.shape[1:]),
                trip_spec(singles.shape[1:]),
                trip_spec((1, size)),
            ],
            out_specs=[
                trip_spec((3, size, size)),
                trip_spec((3, size, size)),
                trip_spec((2, size, size)),
            ],
        ),
        out_shape=[
            jax.ShapeDtypeStruct((trips, 3, size, size), jnp.float32),
            jax.ShapeDtypeStruct((trips, 3, size, size), jnp.float32),
            jax.ShapeDtypeStruct((trips, 2, size, size), jnp.float32),
        ],
        compiler_params=pltpu.CompilerParams(dimension_semantics=("arbitrary",)),
        cost_estimate=pl.CostEstimate(
            flops=12 * trips * size**3, bytes_accessed=8 * trips * size**2 * 4, transcendentals=0
        ),
        name="prepare",
    )(widths, gap, left, right, singles, levels.reshape(trips, 1, size))


def energy_kernel(
    meta, levels_s, singles_s,
    own0, own1, own2, far0, far1, far2, tno, left_t, right_t, columns, singles,
    out,
    weights, exch, next_weights, next_exch, connected_s, outer_s, ix,
):
    step = pl.program_id(0)
    trips = levels_s.shape[0]
    t = jnp.maximum(step - 1, 0)
    width = meta[3 * trips + t]
    next_width = meta[3 * trips + jnp.minimum(step, trips - 1)]
    rep = meta[4 * trips]
    own = (own0, own1, own2)
    far = (far0, far1, far2)
    size = tno.shape[2]
    half_dom = tno.shape[1] // 2
    lanes = own0.shape[2]
    pieces = half_dom // lanes
    pno = (own0.shape[1] * 2) // (2 * pieces + 1)
    part = pno // 2
    pairs = STEP // 2

    def stacked(refs):
        rows = []
        for ref in refs:
            cols = [ref[0, k * pno : (k + 1) * pno, :] for k in range(pieces)]
            rows.append(jnp.concatenate(cols, axis=1))
        return jnp.concatenate(rows, axis=0)

    def project():
        inter = jnp.dot(
            stacked(own),
            tno[0, pl.ds(rep * half_dom, half_dom), :],
            preferred_element_type=jnp.float32,
        )
        inter += jnp.dot(
            stacked(far),
            tno[0, pl.ds((1 - rep) * half_dom, half_dom), :],
            preferred_element_type=jnp.float32,
        )
        lane = lax.broadcasted_iota(jnp.int32, inter.shape, 1)
        inter = jnp.where(lane < next_width, inter, 0.0).astype(jnp.bfloat16)
        for x in range(3):
            mine = own[x][0, pieces * pno : pieces * pno + part, :]
            other = far[x][0, pieces * pno : pieces * pno + part, :]
            ix[x, pl.ds(rep * part, part), :] = mine
            ix[x, pl.ds((1 - rep) * part, part), :] = other
        for x in range(3):
            inter_x = inter[x * pno : (x + 1) * pno, :]
            halfway = dot_tn(inter_x, ix[x]).astype(jnp.bfloat16)
            next_weights[x] = dot_tt(inter_x, halfway[:, :pno]).astype(jnp.bfloat16)
            next_exch[x] = dot_tt(inter_x, halfway[:, pno:])

    single2 = singles[0, 2:3, :]
    spots = ((0, 256), (128, 384), (512, 640))

    def with_rows(m):
        def connect(side, i):
            b0 = i * STEP
            right_x = [right_t[0, x, :m, :].astype(jnp.bfloat16) for x in range(3)]
            left_x = [left_t[0, x, pl.ds(b0, STEP), :] for x in range(3)]

            def product(x, j):
                row = jnp.broadcast_to(left_x[x][j : j + 1, :], (m, size)).astype(jnp.bfloat16)
                return right_x[x] * row

            for group in range(0, pairs, GROUP):
                khatri = jnp.concatenate(
                    [
                        jnp.concatenate(
                            [
                                product(0, j), product(1, j), product(0, j + 1), product(1, j + 1),
                                product(2, j), product(2, j + 1),
                            ],
                            axis=1,
                        )
                        for j in range(2 * group, 2 * (group + GROUP), 2)
                    ],
                    axis=0,
                )
                both = jnp.dot(khatri, weights[...], preferred_element_type=jnp.float32)
                for k in range(GROUP):
                    connected_s[side, group + k, :m, :] = both[k * m : (k + 1) * m, :]
            for j in range(STEP):
                column = exch[2, :m, b0 + j : b0 + j + 1]
                outer_s[side, j, :m, :] = jnp.broadcast_to(column, (m, size))

        def energies(side, i, total):
            b0 = i * STEP
            exch0_rows = exch[0, pl.ds(b0, STEP), :]
            for j in range(STEP):
                connected = connected_s[side, j // 2, :m, (j % 2) * size : (j % 2 + 1) * size]
                complete = connected + singles_s[t, 1, b0 + j] * exch[1, :m, :]
                complete += columns[0, 0, :m, :] * exch0_rows[j : j + 1, :]
                complete += outer_s[side, j, :m, :] * single2
                term = connected * complete / (columns[0, 1, :m, :] + levels_s[t, b0 + j])
                total += jnp.sum(term.reshape(m // 8, 8, size), axis=0)
            return total

        steps = m // STEP
        total = jnp.zeros((8, size), jnp.float32)
        connect(0, 0)
        for i in range(steps):
            total = energies(i % 2, i, total)
            if i + 1 < steps:
                connect((i + 1) % 2, i + 1)
            if i == 1:
                project()
        out[0] = total

    @pl.when(step == 0)
    def _():
        weights[...] = jnp.zeros(weights.shape, weights.dtype)
        project()

    @pl.when(step > 0)
    def _():
        for x in range(3):
            amps = next_weights[x]
            weights[spots[x][0] : spots[x][0] + size, :size] = amps
            weights[spots[x][1] : spots[x][1] + size, size:] = amps
            exch[x] = next_exch[x]
        needed = (width + 15) // 16 * 16
        for m in range(size // 2, size + 1, 16):
            pl.when(needed == m)(lambda m=m: with_rows(m))


def triplet_energies(meta, own, far, tno, left_t, right_t, columns, singles, levels):
    trips, _, size = tno.shape
    slot = own.shape[1:]
    pno = slot[0] * 2 // (tno.shape[1] // slot[1] + 1)

    def ahead(s):
        return jnp.minimum(s, trips - 1)

    def behind_spec(shape):
        return pl.BlockSpec(
            (1, *shape), lambda s, *_: (jnp.maximum(s - 1, 0),) + (0,) * len(shape)
        )

    def pair_spec(x):
        return pl.BlockSpec((1, *slot), lambda s, meta, *_: (meta[3 * ahead(s) + x], 0, 0))

    return pl.pallas_call(
        energy_kernel,
        grid_spec=pltpu.PrefetchScalarGridSpec(
            num_scalar_prefetch=3,
            grid=(trips + 1,),
            in_specs=[pair_spec(x) for x in range(3)]
            + [pair_spec(x) for x in range(3)]
            + [
                pl.BlockSpec((1, *tno.shape[1:]), lambda s, *_: (ahead(s), 0, 0)),
                behind_spec(left_t.shape[1:]),
                behind_spec(right_t.shape[1:]),
                behind_spec(columns.shape[1:]),
                behind_spec(singles.shape[1:]),
            ],
            out_specs=behind_spec((8, size)),
            scratch_shapes=[
                pltpu.VMEM((6 * size, 2 * size), jnp.bfloat16),
                pltpu.VMEM((3, size, size), jnp.float32),
                pltpu.VMEM((3, size, size), jnp.bfloat16),
                pltpu.VMEM((3, size, size), jnp.float32),
                pltpu.VMEM((2, STEP // 2, size, 2 * size), jnp.float32),
                pltpu.VMEM((2, STEP, size, size), jnp.float32),
                pltpu.VMEM((3, pno, 2 * pno), jnp.bfloat16),
            ],
        ),
        out_shape=jax.ShapeDtypeStruct((trips, 8, size), jnp.float32),
        compiler_params=pltpu.CompilerParams(dimension_semantics=("arbitrary",)),
        name="energy",
    )(meta, levels, singles, own, own, own, far, far, far, tno, left_t, right_t, columns, singles)


def test_entry(meta, own, far, tno, left, right, singles, levels, gap):
    trips = tno.shape[0]
    ready = prepare(meta[3 * trips : 4 * trips], gap, left, right, singles, levels)
    return jnp.sum(triplet_energies(meta, own, far, tno, *ready, singles, levels), axis=(1, 2))


def body(
    triplet_pairs, tno_width, pair_width, pair_coeff, pair_amps, pair_exch, tno_coeff,
    int_left, int_right, singles, tno_energy, gap,
):
    owners_n = lax.axis_size("pair")
    reps = lax.axis_size("rep")
    pair_dev, pno, _ = pair_coeff.shape
    rep = lax.axis_index("rep")
    references = triplet_pairs.reshape(-1)
    owners = references // pair_dev
    peers = owners_n * reps
    wide = 128
    peer = lax.broadcasted_iota(jnp.int32, (1, peers, wide), 1) // reps
    at_peer = owners[:, None, None] == peer
    wanted = jnp.sum(jnp.where(at_peer, (references % pair_dev + 1)[:, None, None], 0), axis=0)
    asked = lax.all_to_all(wanted[:, None, :], BOTH, 0, 0, tiled=True).reshape(peers, wide)

    kept = jnp.arange(pno, dtype=jnp.int32)[None, :] < pair_width[:, None]
    kept = kept[:, :, None] & kept[:, None, :]
    zero = jnp.zeros((), pair_amps.dtype)
    blocks = jnp.concatenate(
        [jnp.where(kept, pair_amps, zero), jnp.where(kept, pair_exch, zero)], axis=2
    )
    sent = send_slots(rep[None].astype(jnp.int32), asked, pair_coeff, blocks, reps)
    got = lax.all_to_all(sent, "pair", 0, 0, tiled=True)
    ready = prepare(tno_width, gap, int_left, int_right, singles, tno_energy)
    got = pltpu.with_memory_space_constraint(got, pltpu.HBM)
    far = lax.ppermute(got, "rep", [(0, 1), (1, 0)])
    far = pltpu.with_memory_space_constraint(far, pltpu.HBM)

    meta = jnp.concatenate([owners, tno_width, rep[None].astype(jnp.int32)])
    partial = triplet_energies(meta, got, far, tno_coeff, *ready, singles, tno_energy)
    energies = jnp.sum(partial, axis=(1, 2))

    shares = jnp.repeat(energies / 3.0, 3)
    shares = jnp.sum(jnp.where(at_peer, shares[:, None, None], 0.0), axis=0)
    shares = lax.all_to_all(shares[:, None, :], BOTH, 0, 0, tiled=True).reshape(peers, wide)
    here = asked == lax.broadcasted_iota(jnp.int32, (peers, wide), 1) + 1
    pair_energy = jnp.sum(jnp.where(here, shares, 0.0), axis=0)[:pair_dev]
    return (energies, pair_energy)


def solution(mesh):
    both = P(BOTH)
    pair = P("pair")
    placed = (both, both, pair, pair, pair, pair, both, both, both, both, both, both)
    return jax.shard_map(
        body, mesh=mesh, in_specs=placed, out_specs=(both, pair), check_vma=False
    )
```
